32 devices in a mesh: rep: 1 (over z), r: 4 (over y), s: 8 (over x, core).
Axes of the slice: x: 4, y: 4, z: 1, core: 2. Of those that a mesh axis runs over, the one named last changes fastest.
The devices are a block of a 4x4x8 slice.
Arguments:
- x: bfloat16 [32, 4096, 896], P(('rep', 'r', 's'))
- dy: bfloat16 [32, 4096, 896], P(('rep', 'r', 's'))
- w_gate: bfloat16 [2, 896, 2304], P(None, 's')
- w_up: bfloat16 [2, 896, 2304], P(None, 's')
- w_down: bfloat16 [2, 2304, 896], P(None, 's')
- m_w_gate: float32 [2, 896, 2304], P(None, 's')
- m_w_up: float32 [2, 896, 2304], P(None, 's')
- m_w_down: float32 [2, 2304, 896], P(None, 's')
- v_w_gate: float32 [2, 896, 2304], P(None, 's')
- v_w_up: float32 [2, 896, 2304], P(None, 's')
- v_w_down: float32 [2, 2304, 896], P(None, 's')
Outputs:
- output 1: bfloat16 [2, 896, 2304], P('rep', 's')
- output 2: bfloat16 [2, 896, 2304], P('rep', 's')
- output 3: bfloat16 [2, 2304, 896], P('rep', 's')
- output 4: float32 [2, 896, 2304], P('rep', 's')
- output 5: float32 [2, 896, 2304], P('rep', 's')
- output 6: float32 [2, 2304, 896], P('rep', 's')
- output 7: float32 [2, 896, 2304], P('rep', 's')
- output 8: float32 [2, 896, 2304], P('rep', 's')
- output 9: float32 [2, 2304, 896], P('rep', 's')
All inputs are finite; a program needn't handle non-finite values.
Results may differ from the reference program's by a relative error of at most 0.022.
Values are sent between devices in bfloat16 or wider.
A program may use at most 768 MiB of HBM per device.

```python
import jax
import jax.numpy as jnp
from jax import lax

SEQUENCES = 32
TOKENS = 4096
D = 896
FF = 2304
LAYERS = 2
NAMES = ("w_gate", "w_up", "w_down")
SHAPES = {"w_gate": (LAYERS, D, FF), "w_up": (LAYERS, D, FF), "w_down": (LAYERS, FF, D)}


def bump(key, n, height):
    away = (jnp.arange(n, dtype=jnp.int32) - jax.random.randint(key, (), 0, n, jnp.int32)) % n
    return jnp.where(away < n // 8, height, 1.0)


def together(key, own, strength):
    shared = jax.random.normal(key, own.shape[1:], jnp.float32)
    return (own + strength * shared) * lax.rsqrt(1 + strength * strength)


def setup_inputs(seed: int = 0, part: int = 0) -> dict:
    kx, kdy, ka, kb, kz, kf, kh, kl, *keys = jax.random.split(jax.random.key(seed), 8 + 3 * len(NAMES))
    kx, kdy, ka, kb = (jax.random.fold_in(k, part) for k in (kx, kdy, ka, kb))
    kw, km, kv = (keys[i::3] for i in range(3))
    shape = (SEQUENCES, TOKENS, D)
    much_x, much_dy = jax.random.uniform(kz, (2,), jnp.float32, 0.0, 1.0)
    loud = 2.0 ** jax.random.uniform(jax.random.fold_in(kz, 1), (), jnp.float32, -1.0, 2.0)
    layers = 2.0 ** jax.random.uniform(kl, (LAYERS, 1, 1), jnp.float32, -1.0, 1.0)
    x = together(ka, jax.random.normal(kx, shape, jnp.float32), much_x) * bump(kf, D, 4.0)
    dy = together(kb, jax.random.normal(kdy, shape, jnp.float32), much_dy)
    drawn = {"x": x.astype(jnp.bfloat16), "dy": (loud * dy * (SEQUENCES * TOKENS) ** -0.5).astype(jnp.bfloat16)}
    for key, name in zip(kw, NAMES, strict=True):
        w = jax.random.normal(key, SHAPES[name], jnp.float32) * SHAPES[name][1] ** -0.5
        drawn[name] = (w * {"w_gate": 1.0, "w_up": bump(kh, FF, 4.0), "w_down": layers}[name]).astype(jnp.bfloat16)
    for key, name in zip(km, NAMES, strict=True):
        drawn[f"m_{name}"] = 0.1 * jax.random.normal(key, SHAPES[name], jnp.float32)
    for key, name in zip(kv, NAMES, strict=True):
        drawn[f"v_{name}"] = jax.random.uniform(key, SHAPES[name], jnp.float32, 0.005, 0.015)
    return drawn


def matmul(a, w):
    return jnp.dot(a, w, preferred_element_type=jnp.float32).astype(jnp.bfloat16)


def normed(h):
    wide = h.astype(jnp.float32)
    scale = lax.rsqrt(jnp.mean(wide**2, -1, keepdims=True) + 1e-6)
    return (wide * scale).astype(jnp.bfloat16)


def layer(h, w):
    a = normed(h)
    gate = jnp.dot(a, w["w_gate"], preferred_element_type=jnp.float32)
    up = jnp.dot(a, w["w_up"], preferred_element_type=jnp.float32)
    return h + matmul((jax.nn.silu(gate) * up).astype(jnp.bfloat16), w["w_down"])


def adamw(w, m, v, g):
    m = 0.9 * m + 0.1 * g
    v = 0.95 * v + 0.05 * g * g
    step = m * lax.rsqrt(v + 1e-8) + 0.1 * w
    return (w - 0.02 * step).astype(jnp.bfloat16), m, v


def clipped(gradients, sum_of_squares, count):
    factor = jnp.minimum(1.0, 0.5 * lax.rsqrt(sum_of_squares / count + 1e-30))
    return [g * factor for g in gradients]


def stack(weights, h):
    return lax.scan(lambda h, w: (layer(h, w), None), h, weights)[0]


def reference(x, dy, w_gate, w_up, w_down, m_w_gate, m_w_up, m_w_down, v_w_gate, v_w_up, v_w_down):
    weights = dict(zip(NAMES, (w_gate, w_up, w_down), strict=True))

    def take(so_far, sequence):
        h, by_y = sequence
        _, back = jax.vjp(lambda w: stack(w, h), weights)
        return jax.tree.map(lambda total, term: total + term.astype(jnp.float32), so_far, back(by_y)[0]), None

    none_yet = {name: jnp.zeros(w.shape, jnp.float32) for name, w in weights.items()}
    by_weights, _ = lax.scan(take, none_yet, (x, dy))
    gradients = [by_weights[name].astype(jnp.bfloat16).astype(jnp.float32) for name in NAMES]
    gradients = clipped(gradients, sum(jnp.sum(g * g) for g in gradients), sum(g.size for g in gradients))
    new = [
        adamw(w.astype(jnp.float32), m, v, g)
        for w, m, v, g in zip((w_gate, w_up, w_down), (m_w_gate, m_w_up, m_w_down), (v_w_gate, v_w_up, v_w_down), gradients, strict=True)
    ]
    return tuple(one[which] for which in range(3) for one in new)
```

```python
import jax
import jax.numpy as jnp
from jax import lax
from jax.experimental import pallas as pl
from jax.experimental.pallas import tpu as pltpu
from jax.sharding import PartitionSpec as P

F32, BF16 = jnp.float32, jnp.bfloat16
MESH = pl.DeviceIdType.MESH
DMA = pltpu.SemaphoreType.DMA
ANY = pl.BlockSpec(memory_space=pl.ANY)
VMEM_LIMIT = 63 * 2**20
LANES = 128
WIDE, NARROW = 512, 256


def dot(a, b):
    return jnp.dot(a, b, preferred_element_type=F32)


def dot_nt(a, b):
    return lax.dot_general(a, b, (((1,), (1,)), ((), ())), preferred_element_type=F32)


def params(**more):
    return pltpu.CompilerParams(vmem_limit_bytes=VMEM_LIMIT, dimension_semantics=("arbitrary", "arbitrary"), **more)


def shape(*dims, dtype=BF16):
    return jax.ShapeDtypeStruct(dims, dtype)


def block(dims, index, **more):
    return pl.BlockSpec(dims, index, **more)


def fixed(*dims):
    return pl.BlockSpec(dims, lambda *_: (0,) * len(dims), pipeline_mode=pl.Buffered(1))


def span(i, size, tile=16):
    return pl.ds(pl.multiple_of(i * size, tile), size)


def rms(wide):
    return lax.rsqrt(jnp.mean(wide * wide, -1, keepdims=True) + 1e-6)


def normed(wide):
    return (wide * rms(wide)).astype(BF16)


class Place:
    def __init__(self, sizes):
        self.shards, self.groups = sizes["s"], sizes["r"]
        self.me, self.y = lax.axis_index("s"), lax.axis_index("r")
        self.c = lax.rem(self.me, 2)
        self.right, self.left, self.partner = {"s": self.shard(1)}, {"s": self.shard(-1)}, {"s": self.me + 1 - 2 * self.c}
        self.above, self.below = self.group(1), self.group(-1)
        self.up, self.down = {"r": self.above}, {"r": self.below}
        self.around = [self.left, self.right, self.partner, self.up, self.down]

    def shard(self, chips, other=False):
        s = lax.rem(self.me + 2 * chips + self.shards, self.shards)
        return s + 1 - 2 * self.c if other else s

    def group(self, steps):
        return lax.rem(self.y + steps + self.groups, self.groups)


def greet(devices):
    barrier = pltpu.get_barrier_semaphore()
    for device in devices:
        pl.semaphore_signal(barrier, inc=1, device_id=device, device_id_type=MESH)
    pl.semaphore_wait(barrier, len(devices))


class Copies:
    def _copy(self, name, table):
        i = list(table).index(name)
        src, dst, device = table[name]
        return pltpu.make_async_remote_copy(
            src_ref=src, dst_ref=dst, send_sem=self.send.at[i], recv_sem=self.recv.at[i], device_id=device, device_id_type=MESH
        )

    def start(self, *names):
        table = self.table()
        for name in names:
            self._copy(name, table).start()

    def arrived(self, *names):
        table = self.table()
        for name in names:
            self._copy(name, table).wait_recv()

    def sent(self):
        table = self.table()
        for name in table:
            self._copy(name, table).wait_send()


class Gather(Copies):
    N = 17

    def __init__(self, place, own, whole, part, send, recv):
        self.p, self.own, self.whole, self.part, self.send, self.recv = place, own, whole, part, send, recv

    def table(self):
        p, part = self.p, self.part
        have, lack = lax.rem(p.y, 2), 1 - lax.rem(p.y, 2)
        left, right, far = (p.shard(i) for i in (-1, 1, 2))
        mine = part(p.me, have)
        same = lambda device, *which: (part(*which), part(*which), device)
        table = {
            "left": (self.own(have), mine, p.right),
            "right": (self.own(have), mine, p.left),
            "far0": same(p.right, left, have, 0),
            "far1": same(p.left, right, have, 1),
            "up": same(p.up, right, have),
            "down": same(p.down, left, have),
            "far up": same(p.up, far, have, 0),
            "far down": same(p.down, far, have, 1),
            "my own": (self.own(None), self.whole, p.partner),
        }
        for name, *which in (
            ("my left", left, have),
            ("my right", right, have),
            ("my far0", far, have, 0),
            ("my far1", far, have, 1),
            ("my up", right, lack),
            ("my down", left, lack),
            ("my far up", far, lack, 0),
            ("my far down", far, lack, 1),
        ):
            table[name] = same(p.partner, *which)
        return table

    def _pass(self, *chains):
        for first, *rest in chains:
            self.arrived(first)
            self.start(*rest)

    def first(self):
        self.start("left", "right", "my own")

    def relay(self):
        self._pass(("left", "far0", "down", "my left"), ("right", "far1", "up", "my right"))

    def share(self):
        self._pass(("far0", "far up", "my far0"), ("far1", "far down", "my far1"))

    def collect(self):
        self._pass(*((name, "my " + name) for name in ("up", "down", "far up", "far down")))

    def complete(self):
        self.arrived(*(name for name in self.table() if name.startswith("my ")))


def each(rows, one, size=16):
    @pl.loop(0, rows // size)
    def _(i):
        one(span(i, size))


class Sum(Copies):
    N = 14

    @staticmethod
    def scratch(groups, rows, cols):
        return [pltpu.VMEM((n, 2, rows, cols), BF16) for n in (4, 3, 2, 1, groups)] + [DMA((Sum.N,))] * 2

    def __init__(self, place, mine, theirs, out, squares, scratch):
        self.p, self.mine, self.theirs, self.out, self.squares = place, mine, theirs, out, squares
        self.other, self.sums, self.got, self.through, self.groups, self.send, self.recv = scratch

    def table(self):
        p, sums, got, through, groups = self.p, self.sums, self.got, self.through, self.groups
        mine, below, above = groups.at[p.y], groups.at[p.below, 0], groups.at[p.above, 1]
        table = {i: (self.theirs(i), self.other.at[i], p.partner) for i in range(4)}
        table |= {
            "far0": (sums.at[2, 0], through.at[0, 0], p.right),
            "far1": (sums.at[2, 1], through.at[0, 1], p.left),
            "near1": (sums.at[0, 1], got.at[0, 1], p.right),
            "near0": (sums.at[1, 0], got.at[1, 0], p.left),
            "last0": (sums.at[0, 0], got.at[0, 0], p.right),
            "last1": (sums.at[1, 1], got.at[1, 1], p.left),
            "up": (mine, mine, p.up),
            "down": (mine, mine, p.down),
            "relay0": (below, below, p.up),
            "relay1": (above, above, p.down),
        }
        return table

    def _total(self, terms, half, r):
        total = terms[0](half, r).astype(F32)
        for term in terms[1:]:
            total += term(half, r).astype(F32)
        return total.astype(BF16)

    def _own(self, chips):
        return [lambda half, r: self.mine(chips, half, r), lambda half, r: self.other[chips, half, r, :]]

    def _ready(self, dst, terms, half):
        def one(r):
            dst[half, r, :] = self._total(terms, half, r)

        each(dst.shape[1], one)

    def exchange(self):
        self.start(2, 1, 3, 0)

    def far(self):
        self.arrived(2)
        for half in range(2):
            self._ready(self.sums.at[2], self._own(2), half)
        self.start("far0", "far1")
        self.arrived(1)
        self._ready(self.sums.at[0], self._own(1), 1)
        self.start("near1")
        self.arrived(3)
        self._ready(self.sums.at[1], self._own(3), 0)
        self.start("near0")

    def near(self):
        through = lambda half, r: self.through[0, half, r, :]
        self.arrived("far0")
        self._ready(self.sums.at[0], self._own(1) + [through], 0)
        self.start("last0")
        self.arrived("far1")
        self._ready(self.sums.at[1], self._own(3) + [through], 1)
        self.start("last1")

    def across(self):
        self.arrived(0, "near1", "near0", "last0", "last1")
        got = [lambda half, r, i=i: self.got[i, half, r, :] for i in range(2)]
        for half in range(2):
            self._ready(self.groups.at[self.p.y], self._own(0) + got, half)
        self.start("up", "down")

    def relay(self):
        self.arrived("up")
        self.start("relay0")
        self.arrived("down")
        self.start("relay1")

    def finish(self):
        self.arrived("relay0", "relay1")
        terms = [lambda half, r, i=i: self.groups[i, half, r, :] for i in range(self.groups.shape[0])]
        for half in range(2):

            def one(r):
                g = self._total(terms, half, r)
                self.out[half, r, :] = g
                g = g.astype(F32)
                g = (g * g).reshape(2, -1, g.shape[1])
                g = g[0] + g[1]
                self.squares[...] += sum(g[:, i : i + LANES] for i in range(0, g.shape[1], LANES))

            each(self.out.shape[1], one)

    def stages(self):
        return self.exchange, self.far, self.near, self.across, self.relay, self.finish


def scheduled(phase, t, nt, last, plan, do):
    table = {}
    for item, steps in plan.items():
        for stage, at in enumerate(steps):
            table.setdefault(at, []).append((item, stage))
    for p in range(last // nt + 1):
        steps = [i for i in range(nt) if p * nt + i in table]
        if steps:

            @pl.when(phase == p)
            def _():
                for i in steps:

                    @pl.when(t == i)
                    def _():
                        for one in table[p * nt + i]:
                            do(*one)

    return [one for at in sorted(table) if at > last for one in reversed(table[at])]


def after(first, offsets):
    return [first + i for i in offsets]


def columns(first, width):
    def part(ref, rows):
        def one(s, half, q=None):
            start, size = (first, width) if q is None else (first + q * (width // 2), width // 2)
            return ref.at[half, span(s, rows), pl.ds(start, size)]

        return one

    return part


def down_part(ref, rows):
    def one(s, half, q=None):
        cols = {None: pl.ds(0, ref.shape[1]), 0: pl.ds(0, WIDE), 1: pl.ds(WIDE, ref.shape[1] - WIDE)}[q]
        return ref.at[span(2 * s + half, rows // 2), cols]

    return one


def forward(sizes, x, wg, wu, wd, tb=1024, sub=256):
    t_, d = x.shape
    rows_d, f = wg.shape[1:]
    rows_f = wd.shape[1]
    nf, nt = f // WIDE, t_ // tb
    rest = nf * WIDE
    deep = f - rest + nf // 2 * WIDE
    last = (nf + 3) * nt - 1
    plan = {0: [0, 2, 4, 4], 1: [0, 3, 5, 7]}
    plan |= {k: after(at, (0, 4, 6, 8)) for k, at in enumerate((2, 3, 6, 9, 12, 15, 18), 2)}
    for k, steps in plan.items():
        steps.append((k + 1) * nt if k < nf + 2 else last + 1)

    def kernel(x_ref, wg_ref, wu_ref, wd_ref, gate_ref, up_ref, gate_n_ref, up_n_ref, h_ref, an_ref, a_ref, hid_ref, wd0_ref, wd1_ref, gu1_ref, *scratch):
        hid_all, a_all, wgu, narrow, wdv, mine_gu, mine_w, local, kept, send, recv = scratch
        phase, t = pl.program_id(0), pl.program_id(1)
        step = phase * nt + t
        place = Place(sizes)
        mine_d, mine_f = span(place.me, rows_d), span(place.me, rows_f)

        def narrow_part(s, half, q=None):
            start, size = (half * NARROW, NARROW) if q is None else (half * NARROW + q * LANES, LANES)
            return narrow.at[span(s, rows_d), pl.ds(pl.multiple_of(start, LANES), size)]

        def gate_up(k, ref, first, width, own=None):
            part = columns(first, width)(ref, rows_d)
            whole = ref.at[:, mine_d, pl.ds(first, width)]
            if own is None:
                source = lambda half: whole if half is None else part(place.me, half)
            else:
                source = lambda half: own.at[slice(None) if half is None else half, :, pl.ds(first, width)]
            return Gather(place, source, whole, part, send.at[k], recv.at[k])

        def down(k, ref, own=None):
            part, whole = down_part(ref, rows_f), ref.at[mine_f, :]
            if own is None:
                source = lambda half: whole if half is None else part(place.me, half)
            else:
                source = lambda half: own if half is None else own.at[span(half, rows_f // 2), :]
            return Gather(place, source, whole, part, send.at[k], recv.at[k])

        def gather(k):
            if k == 0:
                whole = narrow.at[mine_d, :]
                own = lambda half: whole if half is None else narrow_part(place.me, half)
                return Gather(place, own, whole, narrow_part, send.at[k], recv.at[k])
            if k <= nf:
                return gate_up(k, wgu, (k - 1) * WIDE, WIDE)
            return {
                nf + 1: lambda: down(k, wdv),
                nf + 2: lambda: down(k, wd1_ref, mine_w),
                nf + 3: lambda: gate_up(k, gu1_ref, 0, f - deep, mine_gu),
                nf + 4: lambda: gate_up(k, gu1_ref, f - deep, deep, mine_gu),
            }[k]()

        def locals_():
            out = []
            for i, ref in enumerate((wg_ref, wu_ref)):
                out.append((ref.at[0, :, pl.ds(rest, NARROW)], narrow.at[mine_d, pl.ds(i * NARROW, NARROW)]))
            for i, ref in enumerate((wg_ref, wu_ref)):
                out.append((ref.at[0, :, pl.ds(0, rest)], wgu.at[i, mine_d, :]))
            out.append((wd_ref.at[0], wdv.at[mine_f, :]))
            out.append((wd_ref.at[1], mine_w))
            for i, ref in enumerate((wg_ref, wu_ref)):
                out.append((ref.at[1], mine_gu.at[i]))
            return [lambda i=i, pair=pair: pltpu.make_async_copy(*pair, local.at[i]) for i, pair in enumerate(out)]

        def keep(k):
            if 0 < k <= nf + 1:
                cols = pl.ds((k - 2) * WIDE, WIDE) if k > 1 else pl.ds(rest, NARROW)
                src, dst = hid_all.at[:, cols], hid_ref.at[:, cols]
            else:
                src, dst = ((a_all, a_ref), (mine_w, wd1_ref.at[mine_f, :]), (mine_gu, gu1_ref.at[:, mine_d, :]), (wdv, wd0_ref))[max(k - nf - 1, 0)]
            return pltpu.make_async_copy(src, dst, kept.at[k])

        @pl.when(step == 0)
        def _():
            for one in locals_():
                one().start()
            greet(place.around)
            for one in locals_()[:4]:
                one().wait()

        def stage_of(k, stage):
            if stage < 4:
                getattr(gather(k), ("first", "relay", "share", "collect")[stage])()
                return
            if k == 1:
                for one in locals_()[4:]:
                    one().wait()
            gather(k).complete()
            if k < nf + 2:
                keep(k).start()
            if k == 1:
                keep(nf + 2).start()
                keep(nf + 3).start()
            if k == nf + 1:
                keep(nf + 4).start()

        late = scheduled(phase, t, nt, last, plan, stage_of)
        def save(gate_ref, up_ref, r, rows, first, gate, up):
            gate_ref[r, :] = gate
            up_ref[r, :] = up
            hid_all[rows, pl.ds(first, gate.shape[1])] = (gate * jax.nn.sigmoid(gate) * up).astype(BF16)

        def blocks(one):
            for i in range(tb // sub):
                one(pl.ds(i * sub, sub), pl.ds(pl.multiple_of(t * tb, tb) + i * sub, sub))

        @pl.when(phase == 0)
        def _():
            def one(r, rows):
                a_all[rows, :] = normed(x_ref[r, :].astype(F32))

            blocks(one)

        @pl.when(phase == 1)
        def _():
            def one(r, rows):
                both = dot(a_all[rows, :], narrow[...])
                save(gate_n_ref, up_n_ref, r, rows, rest, both[:, :NARROW], both[:, NARROW:])

            blocks(one)

        @pl.when((phase > 1) & (phase < nf + 2))
        def _():
            first = pl.multiple_of((phase - 2) * WIDE, WIDE)

            def one(r, rows):
                gate, up = (dot(a_all[rows, :], wgu[i, :, pl.ds(first, WIDE)]) for i in range(2))
                save(gate_ref, up_ref, r, rows, first, gate, up)

            blocks(one)

        @pl.when(phase == nf + 2)
        def _():
            def one(r, rows):
                h = x_ref[r, :] + dot(hid_all[rows, :], wdv[...]).astype(BF16)
                h_ref[r, :] = h
                an_ref[r, :] = normed(h.astype(F32))

            blocks(one)

        @pl.when(step == last)
        def _():
            for k, stage in late:
                stage_of(k, stage)
            for k in plan:
                gather(k).sent()
            for k in range(nf + 5):
                keep(k).wait()

    def during(first, final, width, index=lambda p: 0):
        return block((tb, width), lambda p, t: (jnp.where(p < first, 0, jnp.where(p > final, nt - 1, t)), index(p)))

    rows = block((tb, d), lambda p, t: (jnp.where((p > 0) & (p < nf + 2), nt - 1, t), 0))
    wide = during(2, nf + 1, WIDE, lambda p: jnp.clip(p - 2, 0, nf - 1))
    early, late = during(1, 1, NARROW), during(nf + 2, nf + 2, d)
    return pl.pallas_call(
        kernel,
        grid=(nf + 3, nt),
        in_specs=[rows, ANY, ANY, ANY],
        out_specs=[wide, wide, early, early, late, late] + [ANY] * 5,
        out_shape=[shape(t_, rest, dtype=F32)] * 2
        + [shape(t_, NARROW, dtype=F32)] * 2
        + [shape(t_, d)] * 3
        + [shape(t_, f), shape(f, d), shape(f, d), shape(2, d, f)],
        scratch_shapes=[
            pltpu.VMEM((t_, f), BF16),
            pltpu.VMEM((t_, d), BF16),
            pltpu.VMEM((2, d, rest), BF16),
            pltpu.VMEM((d, 2 * NARROW), BF16),
            pltpu.VMEM((f, d), BF16),
            pltpu.VMEM((2, rows_d, f), BF16),
            pltpu.VMEM((rows_f, d), BF16),
            DMA((8,)),
            DMA((nf + 5,)),
        ]
        + [DMA((nf + 5, Gather.N))] * 2,
        compiler_params=params(collective_id=0, has_side_effects=True),
        name="forward",
    )(x, wg, wu, wd)


def split(gate, up, dh):
    dh = dh.astype(BF16).astype(F32)
    sg = jax.nn.sigmoid(gate)
    si = gate * sg
    return (si * up).astype(BF16), (dh * up * (sg + si * (1 - sg))).astype(BF16), (dh * si).astype(BF16)


def term_blocks(ref, place, rows):
    mine = lambda chips, half, r: ref[half, pl.ds(pl.multiple_of(place.shard(chips) * rows, 16) + r.start, r.size), :]
    return mine, lambda chips: ref.at[:, span(place.shard(chips, True), rows), :]


class Stored:
    def __init__(self, place, ref, own, sems, cols=None):
        self.p, self.ref, self.own, self.sems = place, ref, own, sems
        self.cols = pl.ds(0, ref.shape[-1]) if cols is None else cols

    def block(self, s):
        rows = self.own.shape[2]
        return self.ref.at[pl.ds(2 * s, 2), :, self.cols] if self.ref.shape[0] > 2 else self.ref.at[:, span(s, rows), self.cols]

    def copies(self):
        return [pltpu.make_async_copy(self.block(self.p.shard(i)), self.own.at[i], self.sems.at[i]) for i in range(4)]

    def terms(self):
        return lambda chips, half, r: self.own[chips, half, r, :], lambda chips: self.block(self.p.shard(chips, True))


def parts_of(scratch, count):
    n = len(scratch) // count
    return [scratch[n * k : n * (k + 1)] for k in range(count)]


def zero(*refs):
    for ref in refs:
        ref[...] = jnp.zeros_like(ref)


def backward_top(sizes, a, dy, gu, wd, tb=1024, sub=256):
    t_, d = a.shape
    f = wd.shape[0]
    nf, nt = f // WIDE, t_ // tb
    rows_d = d // sizes["s"]
    done = nf - 1
    plan = {k: after((k + 1) * nt, (0, 1, 3, 4, 6, 7)) for k in range(done)}
    last = (nf + 1) * nt - 1

    def kernel(a_ref, dy_ref, gu_ref, wd_ref, dg_ref, du_ref, last_ref, lastn_ref, od_ref, s_ref, sq_ref, *scratch):
        hid, ag, au, ad, terms = scratch[:5]
        phase, t = pl.program_id(0), pl.program_id(1)
        step = phase * nt + t
        place = Place(sizes)

        def piece(k):
            out = s_ref.at[:, :, pl.ds(k * WIDE, WIDE)]
            return Sum(place, *term_blocks(terms.at[k], place, rows_d), out, sq_ref, parts_of(scratch[5:], done)[k])

        @pl.when(step == 0)
        def _():
            greet(place.around)
            zero(sq_ref)

        scheduled(phase, t, nt, last, plan, lambda k, stage: piece(k).stages()[stage]())

        @pl.when(t == 0)
        def _():
            zero(ag, au, ad)

        def work(width):
            cols = pl.ds(0, width)
            for i in range(tb // sub):
                r = pl.ds(i * sub, sub)
                av, dv = a_ref[r, :], dy_ref[r, :]
                dh = dot_nt(dv, wd_ref[cols, :])
                hid[r, cols], dg_ref[r, cols], du_ref[r, cols] = split(dot(av, gu_ref[0, :, cols]), dot(av, gu_ref[1, :, cols]), dh)
            ad[:, cols] += dot(dy_ref[...].T, hid[:, cols])
            at = a_ref[...].T
            ag[:, cols] += dot(at, dg_ref[:, cols])
            au[:, cols] += dot(at, du_ref[:, cols])

        @pl.when(phase < nf)
        def _():
            work(WIDE)

        @pl.when(phase == nf)
        def _():
            work(NARROW)

        @pl.when(t == nt - 1)
        def _():
            od_ref[...] = ad[...].T.astype(BF16)

        def give(ref, width):
            for i, acc in enumerate((ag, au)):
                ref[i] = acc[:, :width].astype(BF16)

        @pl.when((t == nt - 1) & (phase < done))
        def _():
            give(terms.at[phase], WIDE)

        @pl.when((t == nt - 1) & (phase == done))
        def _():
            give(last_ref, WIDE)

        @pl.when(step == last)
        def _():
            give(lastn_ref, NARROW)
            for k in range(done):
                piece(k).sent()

    rows = block((tb, d), lambda p, t: (t, 0))
    down = block((WIDE, d), lambda p, t: (p, 0))
    chunks = block((tb, WIDE), lambda p, t: (t, p))
    summed = (2, rows_d, done * WIDE)
    return pl.pallas_call(
        kernel,
        grid=(nf + 1, nt),
        in_specs=[rows, rows, block((2, d, WIDE), lambda p, t: (0, 0, p)), down],
        out_specs=[chunks, chunks, fixed(2, d, WIDE), fixed(2, d, NARROW), down, fixed(*summed), fixed(8, LANES)],
        out_shape=[shape(t_, f), shape(t_, f), shape(2, d, WIDE), shape(2, d, NARROW), shape(f, d), shape(*summed), shape(8, LANES, dtype=F32)],
        scratch_shapes=[pltpu.VMEM((tb, WIDE), BF16)]
        + [pltpu.VMEM((d, WIDE), F32)] * 3
        + [pltpu.VMEM((done, 2, d, WIDE), BF16)]
        + Sum.scratch(sizes["r"], rows_d, WIDE) * done,
        compiler_params=params(collective_id=1, has_side_effects=True),
        name="backward_top",
    )(a, dy, gu, wd)


def middle(sizes, dg, du, gu, h, dy, hid, d1, last, last_n, tb=512, sub=256):
    t_, f = dg.shape
    d = h.shape[1]
    nt = t_ // tb
    n_s = sizes["s"]
    rows_d, rows_f = d // n_s, f // n_s // 2
    d1 = d1.reshape(2 * n_s, rows_f, d)
    pieces = [(rows_f, WIDE), (rows_f, d - WIDE), (rows_d, WIDE), (rows_d, NARROW)]
    plan = {k: (0, 1, 4, 5, 7, 8) if k > 1 else (0, 1, 3, 4, 6, 7) for k in range(len(pieces))}

    def kernel(dg_ref, du_ref, gu_ref, h_ref, dy_ref, hid_ref, d1_ref, last_ref, lastn_ref, dh_ref, od_ref, s_ref, sd_ref, sq_ref, *scratch):
        ad, local = scratch[:2]
        t = pl.program_id(1)
        place = Place(sizes)
        wide, narrow = pl.ds(0, WIDE), pl.ds(WIDE, NARROW)
        right = pl.ds(WIDE, d - WIDE)

        def stored(k):
            own = scratch[2 + k]
            sems = local.at[k]
            return (
                lambda: Stored(place, d1_ref, own, sems, wide),
                lambda: Stored(place, d1_ref, own, sems, right),
                lambda: Stored(place, last_ref, own, sems),
                lambda: Stored(place, lastn_ref, own, sems),
            )[k]()

        def piece(k):
            out = (sd_ref.at[:, :, wide], sd_ref.at[:, :, right], s_ref.at[:, :, wide], s_ref.at[:, :, narrow])[k]
            return Sum(place, *stored(k).terms(), out, sq_ref, parts_of(scratch[2 + len(pieces) :], len(pieces))[k])

        @pl.when(t == 0)
        def _():
            zero(ad, sq_ref)
            for k in plan:
                for one in stored(k).copies():
                    one.start()
            greet(place.around)

        @pl.when(t == 1)
        def _():
            for k in plan:
                for one in stored(k).copies():
                    one.wait()

        late = scheduled(pl.program_id(0), t, nt, nt - 1, plan, lambda k, stage: piece(k).stages()[stage]())
        for i in range(tb // sub):
            r = pl.ds(i * sub, sub)
            da = dot_nt(dg_ref[r, :], gu_ref[0]).astype(BF16) + dot_nt(du_ref[r, :], gu_ref[1]).astype(BF16)
            da = da.astype(F32)
            wide_h = h_ref[r, :].astype(F32)
            scale = rms(wide_h)
            back = scale * da - wide_h * (scale * scale * scale * jnp.mean(da * wide_h, -1, keepdims=True))
            dh_ref[r, :] = dy_ref[r, :] + back.astype(BF16)
        ad[...] += dot(dh_ref[...].T, hid_ref[...])

        @pl.when(t == nt - 1)
        def _():
            od_ref[...] = ad[...].T.astype(BF16)
            for k, stage in late:
                piece(k).stages()[stage]()
            for k in plan:
                piece(k).sent()

    rows = lambda n: block((tb, n), lambda p, t: (t, 0))
    summed = (2, rows_d, WIDE + NARROW)
    scratch = [pltpu.VMEM((d, f), F32), DMA((len(pieces), 4))] + [pltpu.VMEM((4, 2) + p, BF16) for p in pieces]
    for p in pieces:
        scratch += Sum.scratch(sizes["r"], *p)
    return pl.pallas_call(
        kernel,
        grid=(1, nt),
        in_specs=[rows(f), rows(f), fixed(2, d, f), rows(d), rows(d), rows(f), ANY, ANY, ANY],
        out_specs=[rows(d), fixed(f, d), fixed(*summed), fixed(2, rows_f, d), fixed(8, LANES)],
        out_shape=[shape(t_, d), shape(f, d), shape(*summed), shape(2, rows_f, d), shape(8, LANES, dtype=F32)],
        scratch_shapes=scratch,
        compiler_params=params(collective_id=2, has_side_effects=True),
        name="middle",
    )(dg, du, gu, h, dy, hid, d1, last, last_n)


def backward_bottom(sizes, a, dy, gate, up, gate_n, up_n, wd, d0, sq1, sq2, tb=1024, sub=256):
    t_, d = a.shape
    f = wd.shape[0]
    nf, nt = f // WIDE, t_ // tb
    n_s = sizes["s"]
    rows_d, rows_f = d // n_s, f // n_s // 2
    d0 = d0.reshape(2 * n_s, rows_f, d)
    pieces = [(rows_d, WIDE)] * nf + [(rows_d, NARROW), (rows_f, WIDE), (rows_f, d - WIDE)]
    last = (nf + 1) * nt - 1
    slow = (0, 1, 4, 6, 9, 11)
    plan = {nf + 1: slow, nf + 2: after(1, slow), 0: after(nt, slow), nf: after(last + 1, (0, 2, 5, 7, 8, 9))}
    plan |= {k: after((k + 1) * nt, (0, 1, 3, 5, 8, 10)) for k in range(1, nf)}

    def kernel(a_ref, dy_ref, gate_ref, up_ref, gaten_ref, upn_ref, wd_ref, d0_ref, sq1_ref, sq2_ref, s_ref, sd_ref, sum_ref, *scratch):
        dgu, acc, own0, own1, terms, terms_n, sq, squares, local, send, recv = scratch[:11]
        phase, t = pl.program_id(0), pl.program_id(1)
        step = phase * nt + t
        place = Place(sizes)
        wide, right = pl.ds(0, WIDE), pl.ds(WIDE, d - WIDE)
        stored = lambda k: Stored(place, d0_ref, (own0, own1)[k], local.at[k], (wide, right)[k])

        def piece(k):
            part = parts_of(scratch[11:], len(pieces))[k]
            if k > nf:
                return Sum(place, *stored(k - nf - 1).terms(), sd_ref.at[:, :, (wide, right)[k - nf - 1]], sq, part)
            out = s_ref.at[:, :, pl.ds(k * WIDE, pieces[k][1])]
            return Sum(place, *term_blocks(terms.at[k] if k < nf else terms_n, place, rows_d), out, sq, part)

        others = [{"s": lax.rem(place.me + i, n_s)} for i in range(1, n_s)]

        def square_copies():
            return [
                pltpu.make_async_remote_copy(
                    src_ref=sq, dst_ref=squares.at[place.me], send_sem=send.at[i], recv_sem=recv.at[i], device_id=to, device_id_type=MESH
                )
                for i, to in enumerate(others)
            ]

        @pl.when(step == 0)
        def _():
            sq[...] = sq1_ref[...] + sq2_ref[...]
            for k in range(2):
                for one in stored(k).copies():
                    one.start()
            greet(others + [place.up, place.down])
            for k in range(2):
                for one in stored(k).copies():
                    one.wait()

        late = scheduled(phase, t, nt, last, plan, lambda k, stage: piece(k).stages()[stage]())

        @pl.when(t == 0)
        def _():
            zero(acc)

        def work(width, gate_ref, up_ref):
            both = pl.ds(0, 2 * width)
            for i in range(tb // sub):
                r = pl.ds(i * sub, sub)
                dh = dot_nt(dy_ref[r, :], wd_ref[pl.ds(0, width), :])
                _, dgu[r, pl.ds(0, width)], dgu[r, pl.ds(width, width)] = split(gate_ref[r, :], up_ref[r, :], dh)
            acc[:, both] += dot(a_ref[...].T, dgu[:, both])

        @pl.when(phase < nf)
        def _():
            work(WIDE, gate_ref, up_ref)

        @pl.when(phase == nf)
        def _():
            work(NARROW, gaten_ref, upn_ref)

        @pl.when((t == nt - 1) & (phase < nf))
        def _():
            for i in range(2):
                terms[phase, i] = acc[:, i * WIDE : (i + 1) * WIDE].astype(BF16)

        @pl.when(step == last)
        def _():
            for i in range(2):
                terms_n[i] = acc[:, i * NARROW : (i + 1) * NARROW].astype(BF16)
            for k, stage in late:
                piece(k).stages()[stage]()
            for one in square_copies():
                one.start()
            squares[place.me] = sq[...]
            for one in square_copies():
                one.wait_recv()
            sum_ref[...] = sum(squares[i] for i in range(n_s))
            for k in range(len(pieces)):
                piece(k).sent()
            for one in square_copies():
                one.wait_send()

    rows = block((tb, d), lambda p, t: (t, 0))
    chunks = block((tb, WIDE), lambda p, t: (jnp.where(p < nf, t, nt - 1), jnp.minimum(p, nf - 1)))
    narrow = block((tb, NARROW), lambda p, t: (jnp.where(p < nf, 0, t), 0))
    lanes = (8, LANES)
    scratch = [pltpu.VMEM((tb, 2 * WIDE), BF16), pltpu.VMEM((d, 2 * WIDE), F32)]
    scratch += [pltpu.VMEM((4, 2) + p, BF16) for p in pieces[nf + 1 :]]
    scratch += [pltpu.VMEM((nf, 2, d, WIDE), BF16), pltpu.VMEM((2, d, NARROW), BF16), pltpu.VMEM(lanes, F32), pltpu.VMEM((n_s,) + lanes, F32)]
    scratch += [DMA((2, 4)), DMA((n_s - 1,)), DMA((n_s - 1,))]
    for p in pieces:
        scratch += Sum.scratch(sizes["r"], *p)
    return pl.pallas_call(
        kernel,
        grid=(nf + 1, nt),
        in_specs=[rows, rows, chunks, chunks, narrow, narrow, block((WIDE, d), lambda p, t: (p, 0)), ANY, fixed(*lanes), fixed(*lanes)],
        out_specs=[fixed(2, rows_d, f), fixed(2, rows_f, d), fixed(*lanes)],
        out_shape=[shape(2, rows_d, f), shape(2, rows_f, d), shape(*lanes, dtype=F32)],
        scratch_shapes=scratch,
        compiler_params=params(collective_id=3, has_side_effects=True),
        name="backward_bottom",
    )(a, dy, gate, up, gate_n, up_n, wd, d0, sq1, sq2)


def update(sizes, weights, m, v, s0, s1, s1_end, sd0, sd1, squares, n=6):
    layers, rows_d, f = weights[0].shape
    rows_f, d = weights[2].shape[1:]
    wide, tall = f // n, rows_f // n
    early = s1.shape[2] // wide
    sd0, sd1 = (one.reshape(rows_f, d) for one in (sd0, sd1))
    count = sizes["s"] * sum(w.size for w in weights)

    def kernel(s0_ref, s1_ref, s1e_ref, sd0_ref, sd1_ref, sq_ref, *refs):
        ins, outs = refs[:9], refs[9:]
        factor = jnp.minimum(1.0, 0.5 * lax.rsqrt(jnp.sum(sq_ref[...], keepdims=True) / count + 1e-30))

        def one(i, layer, g):
            w_ref, m_ref, v_ref = ins[i::3]
            g = g.astype(F32) * factor
            new_m = 0.9 * m_ref[layer] + 0.1 * g
            new_v = 0.95 * v_ref[layer] + 0.05 * g * g
            w = w_ref[layer].astype(F32)
            outs[i][layer] = (w - 0.02 * (new_m * lax.rsqrt(new_v + 1e-8) + 0.1 * w)).astype(BF16)
            outs[i + 3][layer] = new_m
            outs[i + 6][layer] = new_v

        for i in range(2):
            one(i, 0, s0_ref[i])
            one(i, 1, jnp.where(pl.program_id(0) < early, s1_ref[i], s1e_ref[i]))
        one(2, 0, sd0_ref[...])
        one(2, 1, sd1_ref[...])

    across = lambda first, index: block((first, rows_d, wide), lambda p: (0, 0, index(p)))
    whole = [across(layers, lambda p: p)] * 2 + [block((layers, tall, d), lambda p: (0, p, 0))]
    low = block((tall, d), lambda p: (p, 0))
    arrays = (*weights, *m, *v)
    return pl.pallas_call(
        kernel,
        grid=(n,),
        in_specs=[across(2, lambda p: p), across(2, lambda p: jnp.minimum(p, early - 1)), across(2, lambda p: jnp.maximum(p - early, 0)), low, low, fixed(8, LANES)]
        + whole * 3,
        out_specs=whole * 3,
        out_shape=[jax.ShapeDtypeStruct(one.shape, one.dtype) for one in arrays],
        compiler_params=pltpu.CompilerParams(vmem_limit_bytes=VMEM_LIMIT),
        name="update",
    )(s0, s1, s1_end, sd0, sd1, squares, *arrays)


def solution(mesh):
    sizes = dict(mesh.shape)

    def step(x, dy, *arrays):
        weights, m, v = (arrays[i : i + 3] for i in (0, 3, 6))
        x, dy = x[0], dy[0]
        gate, up, gate_n, up_n, h1, a1, a0, hid, wd0, wd1, gu1 = forward(sizes, x, *weights)
        dg, du, last, last_n, d1, s1, sq1 = backward_top(sizes, a1, dy, gu1, wd1)
        dh1, d0, s1_end, sd1, sq2 = middle(sizes, dg, du, gu1, h1, dy, hid, d1, last, last_n)
        s0, sd0, squares = backward_bottom(sizes, a0, dh1, gate, up, gate_n, up_n, wd0, d0, sq1, sq2)
        return tuple(update(sizes, weights, m, v, s0, s1, s1_end, sd0, sd1, squares))

    states, cut = P(("rep", "r", "s"), None, None), P(None, "s", None)
    return jax.shard_map(
        step,
        mesh=mesh,
        in_specs=(states, states) + (cut,) * 9,
        out_specs=(P("rep", "s", None),) * 9,
        check_vma=False,
    )
```

```python
import jax
import jax.numpy as jnp
from jax import lax
from jax.experimental import pallas as pl
from jax.experimental.pallas import tpu as pltpu
from jax.sharding import PartitionSpec as P

F32, BF16 = jnp.float32, jnp.bfloat16
MESH = pl.DeviceIdType.MESH
DMA = pltpu.SemaphoreType.DMA
ANY = pl.BlockSpec(memory_space=pl.ANY)
VMEM_LIMIT = 67043328
LANES = 128
WIDE, NARROW = 512, 256


def dot(a, b):
    return jnp.dot(a, b, preferred_element_type=F32)


def dot_nt(a, b):
    return lax.dot_general(a, b, (((1,), (1,)), ((), ())), preferred_element_type=F32)


def params(**more):
    return pltpu.CompilerParams(vmem_limit_bytes=VMEM_LIMIT, dimension_semantics=("arbitrary", "arbitrary"), **more)


def shape(*dims, dtype=BF16):
    return jax.ShapeDtypeStruct(dims, dtype)


def block(dims, index, **more):
    return pl.BlockSpec(dims, index, **more)


def fixed(*dims):
    return pl.BlockSpec(dims, lambda *_: (0,) * len(dims), pipeline_mode=pl.Buffered(1))


def place_in_grid():
    return pl.program_id(0), pl.program_id(1)


def row_blocks(tb, n):
    return block((tb, n), lambda p, t: (t, 0))


def span(i, size, tile=16):
    return pl.ds(pl.multiple_of(i * size, tile), size)


def rms(wide):
    return lax.rsqrt(jnp.mean(wide * wide, -1, keepdims=True) + 1e-6)


def normed(wide):
    return (wide * rms(wide)).astype(BF16)


class Place:
    def __init__(self, sizes):
        self.shards, self.groups = sizes["s"], sizes["r"]
        self.me, self.y = lax.axis_index("s"), lax.axis_index("r")
        self.c = lax.rem(self.me, 2)
        self.right, self.left, self.partner = {"s": self.shard(1)}, {"s": self.shard(-1)}, {"s": self.me + 1 - 2 * self.c}
        self.above, self.below = self.group(1), self.group(-1)
        self.up, self.down = {"r": self.above}, {"r": self.below}
        self.around = [self.left, self.right, self.partner, self.up, self.down]

    def shard(self, chips, other=False):
        s = lax.rem(self.me + 2 * chips + self.shards, self.shards)
        return s + 1 - 2 * self.c if other else s

    def group(self, steps):
        return lax.rem(self.y + steps + self.groups, self.groups)


def greet(devices):
    barrier = pltpu.get_barrier_semaphore()
    for device in devices:
        pl.semaphore_signal(barrier, inc=1, device_id=device, device_id_type=MESH)
    pl.semaphore_wait(barrier, len(devices))


class Copies:
    def _copy(self, name, table):
        i = list(table).index(name)
        src, dst, device = table[name]
        return pltpu.make_async_remote_copy(
            src_ref=src, dst_ref=dst, send_sem=self.send.at[i], recv_sem=self.recv.at[i], device_id=device, device_id_type=MESH
        )

    def start(self, *names):
        table = self.table()
        for name in names:
            self._copy(name, table).start()

    def arrived(self, *names):
        table = self.table()
        for name in names:
            self._copy(name, table).wait_recv()

    def sent(self):
        table = self.table()
        for name in table:
            self._copy(name, table).wait_send()


class Gather(Copies):
    N = 17

    def __init__(self, place, own, whole, part, send, recv):
        self.p, self.own, self.whole, self.part, self.send, self.recv = place, own, whole, part, send, recv

    def table(self):
        p, part = self.p, self.part
        have, lack = lax.rem(p.y, 2), 1 - lax.rem(p.y, 2)
        left, right, far = (p.shard(i) for i in (-1, 1, 2))
        mine = part(p.me, have)
        same = lambda device, *which: (part(*which), part(*which), device)
        table = {
            "left": (self.own(have), mine, p.right),
            "right": (self.own(have), mine, p.left),
            "far0": same(p.right, left, have, 0),
            "far1": same(p.left, right, have, 1),
            "up": same(p.up, right, have),
            "down": same(p.down, left, have),
            "far up": same(p.up, far, have, 0),
            "far down": same(p.down, far, have, 1),
            "my own": (self.own(None), self.whole, p.partner),
        }
        for name, *which in (
            ("my left", left, have),
            ("my right", right, have),
            ("my far0", far, have, 0),
            ("my far1", far, have, 1),
            ("my up", right, lack),
            ("my down", left, lack),
            ("my far up", far, lack, 0),
            ("my far down", far, lack, 1),
        ):
            table[name] = same(p.partner, *which)
        return table

    def _pass(self, *chains):
        for first, *rest in chains:
            self.arrived(first)
            self.start(*rest)

    def first(self):
        self.start("left", "right", "my own")

    def relay(self):
        self._pass(("left", "far0", "down", "my left"), ("right", "far1", "up", "my right"))

    def share(self):
        self._pass(("far0", "far up", "my far0"), ("far1", "far down", "my far1"))

    def collect(self):
        self._pass(*((name, "my " + name) for name in ("up", "down", "far up", "far down")))

    def complete(self):
        self.arrived(*(name for name in self.table() if name.startswith("my ")))


def each(rows, one, size=16):
    @pl.loop(0, rows // size)
    def _(i):
        one(span(i, size))


class Sum(Copies):
    N = 14

    @staticmethod
    def scratch(groups, rows, cols):
        return [pltpu.VMEM((n, 2, rows, cols), BF16) for n in (4, 3, 2, 1, groups)] + [DMA((Sum.N,))] * 2

    def __init__(self, place, mine, theirs, out, squares, scratch):
        self.p, self.mine, self.theirs, self.out, self.squares = place, mine, theirs, out, squares
        self.other, sums, got, self.through, self.groups, self.send, self.recv = scratch
        self.rightward, self.leftward, self.farther = (sums.at[i] for i in range(3))
        self.got = [got.at[i] for i in range(2)]

    def table(self):
        p, right, left, far, groups = self.p, self.rightward, self.leftward, self.farther, self.groups
        from_left, from_right = self.got
        through = self.through.at[0]
        mine, below, above = groups.at[p.y], groups.at[p.below, 0], groups.at[p.above, 1]
        table = {i: (self.theirs(i), self.other.at[i], p.partner) for i in range(4)}
        table |= {
            "far0": (far.at[0], through.at[0], p.right),
            "far1": (far.at[1], through.at[1], p.left),
            "near1": (right.at[1], from_left.at[1], p.right),
            "near0": (left.at[0], from_right.at[0], p.left),
            "last0": (right.at[0], from_left.at[0], p.right),
            "last1": (left.at[1], from_right.at[1], p.left),
            "up": (mine, mine, p.up),
            "down": (mine, mine, p.down),
            "relay0": (below, below, p.up),
            "relay1": (above, above, p.down),
        }
        return table

    def _total(self, terms, half, r):
        total = terms[0](half, r).astype(F32)
        for term in terms[1:]:
            total += term(half, r).astype(F32)
        return total.astype(BF16)

    def _own(self, chips):
        return [lambda half, r: self.mine(chips, half, r), lambda half, r: self.other[chips, half, r, :]]

    def _ready(self, dst, terms, half):
        def one(r):
            dst[half, r, :] = self._total(terms, half, r)

        each(dst.shape[1], one)

    def exchange(self):
        self.start(2, 1, 3, 0)

    def far(self):
        self.arrived(2)
        for half in range(2):
            self._ready(self.farther, self._own(2), half)
        self.start("far0", "far1")
        self.arrived(1)
        self._ready(self.rightward, self._own(1), 1)
        self.start("near1")
        self.arrived(3)
        self._ready(self.leftward, self._own(3), 0)
        self.start("near0")

    def near(self):
        through = lambda half, r: self.through[0, half, r, :]
        self.arrived("far0")
        self._ready(self.rightward, self._own(1) + [through], 0)
        self.start("last0")
        self.arrived("far1")
        self._ready(self.leftward, self._own(3) + [through], 1)
        self.start("last1")

    def across(self):
        self.arrived(0, "near1", "near0", "last0", "last1")
        got = [lambda half, r, ref=ref: ref[half, r, :] for ref in self.got]
        for half in range(2):
            self._ready(self.groups.at[self.p.y], self._own(0) + got, half)
        self.start("up", "down")

    def relay(self):
        self.arrived("up")
        self.start("relay0")
        self.arrived("down")
        self.start("relay1")

    def finish(self):
        self.arrived("relay0", "relay1")
        terms = [lambda half, r, i=i: self.groups[i, half, r, :] for i in range(self.groups.shape[0])]
        for half in range(2):

            def one(r):
                g = self._total(terms, half, r)
                self.out[half, r, :] = g
                g = g.astype(F32)
                g = (g * g).reshape(2, -1, g.shape[1])
                g = g[0] + g[1]
                self.squares[...] += sum(g[:, i : i + LANES] for i in range(0, g.shape[1], LANES))

            each(self.out.shape[1], one)

    def stages(self):
        return self.exchange, self.far, self.near, self.across, self.relay, self.finish


def scheduled(phase, phases, t, nt, plan, do, part=0, parts=1):
    table = {}
    for item, steps in plan.items():
        for stage, at in enumerate(steps):
            table.setdefault(at, []).append((item, stage))
    for p in range(phases):
        here = {i: table[at] for i in range(nt) if (at := (p * nt + i) * parts + part) in table}
        if here:

            @pl.when(phase == p)
            def _():
                for i, items in here.items():

                    @pl.when(t == i)
                    def _():
                        for one in items:
                            do(*one)


def leftover(plan, last):
    return [one for _, one in sorted(((at, (k, i)) for k, steps in plan.items() for i, at in enumerate(steps) if at > last), key=lambda one: one[0])]


def after(first, offsets):
    return [first + i for i in offsets]


def columns(first, width):
    def part(ref, rows):
        def one(s, half, q=None):
            start, size = (first, width) if q is None else (first + q * (width // 2), width // 2)
            return ref.at[half, span(s, rows), pl.ds(start, size)]

        return one

    return part


def down_part(ref, rows):
    def one(s, half, q=None):
        cols = {None: pl.ds(0, ref.shape[1]), 0: pl.ds(0, WIDE), 1: pl.ds(WIDE, ref.shape[1] - WIDE)}[q]
        return ref.at[span(2 * s + half, rows // 2), cols]

    return one


def forward(sizes, x, wg, wu, wd, tb=1024, sub=256):
    t_, d = x.shape
    rows_d, f = wg.shape[1:]
    rows_f = wd.shape[1]
    nf, nt = f // WIDE, t_ // tb
    rest = nf * WIDE
    last = (nf + 3) * nt - 1
    plan = dict(
        narrow=(0, 2, 4, 4, nt),
        wide0=(0, 3, 5, 7, 2 * nt),
        wide1=(4, 6, 8, 10, 3 * nt),
        wide2=(6, 11, 13, 15, 4 * nt),
        down0=(9, 13, 15, 18, (nf + 2) * nt),
        down1=(12, 16, 19, 21, last + 1),
        gu1=(14, 20, 24, 26, last + 1),
    )

    def kernel(x_ref, wg_ref, wu_ref, wd_ref, gate_ref, up_ref, gate_n_ref, up_n_ref, h_ref, an_ref, a_ref, hid_ref, wd0_ref, wd1_ref, gu1_ref, *scratch):
        hid_all, a_all, wgu, narrow, wdv, mine_gu, mine_w, local, kept, send, recv = scratch
        phase, t = place_in_grid()
        step = phase * nt + t
        place = Place(sizes)
        mine_d, mine_f = span(place.me, rows_d), span(place.me, rows_f)

        def narrow_part(s, half, q=None):
            start, size = (half * NARROW, NARROW) if q is None else (half * NARROW + q * LANES, LANES)
            return narrow.at[span(s, rows_d), pl.ds(pl.multiple_of(start, LANES), size)]

        def gate_up(k, ref, first, width, own=None):
            part = columns(first, width)(ref, rows_d)
            whole = ref.at[:, mine_d, pl.ds(first, width)]
            if own is None:
                source = lambda half: whole if half is None else part(place.me, half)
            else:
                source = lambda half: own.at[slice(None) if half is None else half, :, pl.ds(first, width)]
            return Gather(place, source, whole, part, send.at[k], recv.at[k])

        def down(k, ref, own=None):
            part, whole = down_part(ref, rows_f), ref.at[mine_f, :]
            if own is None:
                source = lambda half: whole if half is None else part(place.me, half)
            else:
                source = lambda half: own if half is None else own.at[span(half, rows_f // 2), :]
            return Gather(place, source, whole, part, send.at[k], recv.at[k])

        def gather(name):
            k = list(plan).index(name)
            if name == "narrow":
                whole = narrow.at[mine_d, :]
                own = lambda half: whole if half is None else narrow_part(place.me, half)
                return Gather(place, own, whole, narrow_part, send.at[k], recv.at[k])
            return dict(
                wide0=lambda: gate_up(k, wgu, 0, WIDE),
                wide1=lambda: gate_up(k, wgu, WIDE, WIDE),
                wide2=lambda: gate_up(k, wgu, 2 * WIDE, rest - 2 * WIDE),
                down0=lambda: down(k, wdv),
                down1=lambda: down(k, wd1_ref, mine_w),
                gu1=lambda: gate_up(k, gu1_ref, 0, f, mine_gu),
            )[name]()

        def locals_():
            out = []
            for i, ref in enumerate((wg_ref, wu_ref)):
                out.append((ref.at[0, :, pl.ds(rest, NARROW)], narrow.at[mine_d, pl.ds(i * NARROW, NARROW)]))
            for i, ref in enumerate((wg_ref, wu_ref)):
                out.append((ref.at[0, :, pl.ds(0, rest)], wgu.at[i, mine_d, :]))
            out.append((wd_ref.at[0], wdv.at[mine_f, :]))
            out.append((wd_ref.at[1], mine_w))
            for i, ref in enumerate((wg_ref, wu_ref)):
                out.append((ref.at[1], mine_gu.at[i]))
            return [lambda i=i, pair=pair: pltpu.make_async_copy(*pair, local.at[i]) for i, pair in enumerate(out)]

        def keep(k):
            if 0 < k <= nf + 1:
                cols = pl.ds((k - 2) * WIDE, WIDE) if k > 1 else pl.ds(rest, NARROW)
                src, dst = hid_all.at[:, cols], hid_ref.at[:, cols]
            else:
                src, dst = ((a_all, a_ref), (mine_w, wd1_ref.at[mine_f, :]), (mine_gu, gu1_ref.at[:, mine_d, :]), (wdv, wd0_ref))[max(k - nf - 1, 0)]
            return pltpu.make_async_copy(src, dst, kept.at[k])

        @pl.when(step == 0)
        def _():
            for one in locals_():
                one().start()
            greet(place.around)
            for one in locals_()[:5]:
                one().wait()

        def stage_of(name, stage):
            if name == "kept":
                keep(stage).start()
                return
            if (name, stage) == ("down1", 0):
                for one in locals_()[5:]:
                    one().wait()
                keep(nf + 2).start()
                keep(nf + 3).start()
            getattr(gather(name), ("first", "relay", "share", "collect", "complete")[stage])()
            if (name, stage) == ("down0", 4):
                keep(nf + 4).start()

        scheduled(phase, nf + 3, t, nt, plan | dict(kept=[(k + 1) * nt for k in range(nf + 2)]), stage_of)
        def save(by_gate_ref, by_up_ref, r, rows, first, gate, up):
            sg = jax.nn.sigmoid(gate)
            si = gate * sg
            by_gate_ref[r, :] = up * (sg + si * (1 - sg))
            by_up_ref[r, :] = si
            hid_all[rows, pl.ds(first, gate.shape[1])] = (si * up).astype(BF16)

        def blocks(one):
            for i in range(tb // sub):
                one(pl.ds(i * sub, sub), span(t * (tb // sub) + i, sub))

        @pl.when(phase == 0)
        def _():
            def one(r, rows):
                a_all[rows, :] = normed(x_ref[r, :].astype(F32))

            blocks(one)

        @pl.when(phase == 1)
        def _():
            def one(r, rows):
                both = dot(a_all[rows, :], narrow[...])
                save(gate_n_ref, up_n_ref, r, rows, rest, both[:, :NARROW], both[:, NARROW:])

            blocks(one)

        @pl.when((phase > 1) & (phase < nf + 2))
        def _():
            first = pl.multiple_of((phase - 2) * WIDE, WIDE)

            def one(r, rows):
                gate, up = (dot(a_all[rows, :], wgu[i, :, pl.ds(first, WIDE)]) for i in range(2))
                save(gate_ref, up_ref, r, rows, first, gate, up)

            blocks(one)

        @pl.when(phase == nf + 2)
        def _():
            def one(i):
                r, rows = span(i, 2 * sub), span(t * (tb // sub // 2) + i, 2 * sub)
                h = x_ref[r, :] + dot(hid_all[rows, :], wdv[...]).astype(BF16)
                h_ref[r, :] = h
                an_ref[r, :] = normed(h.astype(F32))

            pl.loop(0, tb // sub // 2)(one)

        @pl.when(step == last)
        def _():
            for k, stage in leftover(plan, last):
                stage_of(k, stage)
            for k in plan:
                gather(k).sent()
            for k in range(nf + 5):
                keep(k).wait()

    def at(p, t, first, final):
        return jnp.where(p < first, 0, jnp.where(p > final, nt - 1, t))

    def during(first, final, width):
        return block((tb, width), lambda p, t: (at(p, t, first, final), 0))

    rows = block((tb, d), lambda p, t: (jnp.where((p > 0) & (p < nf + 2), nt - 1, t), 0))
    wide = block((None, tb, WIDE), lambda p, t: (jnp.clip(p - 2, 0, nf - 1), at(p, t, 2, nf + 1), 0))
    early, late = during(1, 1, NARROW), during(nf + 2, nf + 2, d)
    return pl.pallas_call(
        kernel,
        grid=(nf + 3, nt),
        in_specs=[rows, ANY, ANY, ANY],
        out_specs=[wide, wide, early, early, late, late] + [ANY] * 5,
        out_shape=[shape(nf, t_, WIDE, dtype=F32)] * 2
        + [shape(t_, NARROW, dtype=F32)] * 2
        + [shape(t_, d)] * 3
        + [shape(t_, f), shape(f, d), shape(f, d), shape(2, d, f)],
        scratch_shapes=[
            pltpu.VMEM((t_, f), BF16),
            pltpu.VMEM((t_, d), BF16),
            pltpu.VMEM((2, d, rest), BF16),
            pltpu.VMEM((d, 2 * NARROW), BF16),
            pltpu.VMEM((f, d), BF16),
            pltpu.VMEM((2, rows_d, f), BF16),
            pltpu.VMEM((rows_f, d), BF16),
            DMA((8,)),
            DMA((nf + 5,)),
        ]
        + [DMA((len(plan), Gather.N))] * 2,
        compiler_params=params(collective_id=0, has_side_effects=True),
        name="forward",
    )(x, wg, wu, wd)


def split(gate, up, dh):
    dh = dh.astype(BF16).astype(F32)
    sg = jax.nn.sigmoid(gate)
    si = gate * sg
    return (si * up).astype(BF16), (dh * up * (sg + si * (1 - sg))).astype(BF16), (dh * si).astype(BF16)


def term_blocks(ref, place, rows):
    mine = lambda chips, half, r: ref[half, pl.ds(pl.multiple_of(place.shard(chips) * rows, 16) + r.start, r.size), :]
    return mine, lambda chips: ref.at[:, span(place.shard(chips, True), rows), :]


class Stored:
    def __init__(self, place, ref, own, sems, cols=None):
        self.p, self.ref, self.own, self.sems = place, ref, own, sems
        self.cols = pl.ds(0, ref.shape[-1]) if cols is None else cols

    def block(self, s):
        rows = self.own.shape[2]
        return self.ref.at[pl.ds(2 * s, 2), :, self.cols] if self.ref.shape[0] > 2 else self.ref.at[:, span(s, rows), self.cols]

    def copies(self):
        return [pltpu.make_async_copy(self.block(self.p.shard(i)), self.own.at[i], self.sems.at[i]) for i in range(4)]

    def terms(self):
        return lambda chips, half, r: self.own[chips, half, r, :], lambda chips: self.block(self.p.shard(chips, True))


def parts_of(scratch, count):
    n = len(scratch) // count
    return [scratch[n * k : n * (k + 1)] for k in range(count)]


def zero(*refs):
    for ref in refs:
        ref[...] = jnp.zeros_like(ref)


def transposed(dst, src):
    @pl.loop(0, src.shape[1] // LANES)
    def _(i):
        dst[span(i, LANES), :] = src[:, span(i, LANES, LANES)].T.astype(BF16)


def backward_top(sizes, a, dy, gu, wd, nf=3, tb=1024, sub=256):
    t_, d = a.shape
    f = wd.shape[0]
    fc, nt = f // nf, t_ // tb
    rows_d = d // sizes["s"]
    done = nf - 1
    last = nf * nt - 1
    plan = {k: after(2 * (k + 1) * nt, (0, 1, 3, 5, 7, 8)) for k in range(done)}

    def kernel(a_ref, dy_ref, gu_ref, wd_ref, dg_ref, du_ref, last_ref, od_ref, s_ref, sq_ref, *scratch):
        hid, ag, au, ad, terms = scratch[:5]
        phase, t = place_in_grid()
        place = Place(sizes)

        def piece(k):
            out = s_ref.at[:, :, pl.ds(k * fc, fc)]
            return Sum(place, *term_blocks(terms.at[k], place, rows_d), out, sq_ref, parts_of(scratch[5:], done)[k])

        @pl.when(phase * nt + t == 0)
        def _():
            greet(place.around)
            zero(sq_ref)

        def stage_of(k, stage):
            piece(k).stages()[stage]()

        scheduled(phase, nf, t, nt, plan, stage_of, 0, 2)

        @pl.when(t == 0)
        def _():
            zero(ag, au, ad)

        for i in range(tb // sub):
            r = pl.ds(i * sub, sub)
            av, dv = a_ref[r, :], dy_ref[r, :]
            hid[r, :], dg_ref[r, :], du_ref[r, :] = split(dot(av, gu_ref[0]), dot(av, gu_ref[1]), dot_nt(dv, wd_ref[...]))
        scheduled(phase, nf, t, nt, plan, stage_of, 1, 2)
        ad[...] += dot(dy_ref[...].T, hid[...])
        at = a_ref[...].T
        ag[...] += dot(at, dg_ref[...])
        au[...] += dot(at, du_ref[...])

        def give(ref):
            for i, acc in enumerate((ag, au)):
                ref[i] = acc[...].astype(BF16)

        @pl.when(t == nt - 1)
        def _():
            transposed(od_ref, ad)

        @pl.when((t == nt - 1) & (phase < done))
        def _():
            give(terms.at[phase])

        @pl.when((t == nt - 1) & (phase == done))
        def _():
            give(last_ref)
            for k, stage in leftover(plan, 2 * last + 1):
                stage_of(k, stage)
            for k in range(done):
                piece(k).sent()

    rows = row_blocks(tb, d)
    down = block((fc, d), lambda p, t: (p, 0))
    chunks = block((tb, fc), lambda p, t: (t, p))
    summed = (2, rows_d, done * fc)
    return pl.pallas_call(
        kernel,
        grid=(nf, nt),
        in_specs=[rows, rows, block((2, d, fc), lambda p, t: (0, 0, p)), down],
        out_specs=[chunks, chunks, fixed(2, d, fc), down, fixed(*summed), fixed(8, LANES)],
        out_shape=[shape(t_, f), shape(t_, f), shape(2, d, fc), shape(f, d), shape(*summed), shape(8, LANES, dtype=F32)],
        scratch_shapes=[pltpu.VMEM((tb, fc), BF16)]
        + [pltpu.VMEM((d, fc), F32)] * 3
        + [pltpu.VMEM((done, 2, d, fc), BF16)]
        + Sum.scratch(sizes["r"], rows_d, fc) * done,
        compiler_params=params(collective_id=1, has_side_effects=True),
        name="backward_top",
    )(a, dy, gu, wd)


def middle(sizes, dg, du, gu, h, dy, hid, d1, last, tb=512, sub=256):
    t_, f = dg.shape
    d = h.shape[1]
    nt = t_ // tb
    n_s = sizes["s"]
    rows_d, rows_f = d // n_s, f // n_s // 2
    d1 = d1.reshape(2 * n_s, rows_f, d)
    pieces = [(rows_f, WIDE), (rows_f, d - WIDE), (rows_d, last.shape[2])]
    plan = {k: (0, 1, 4, 5, 7, nt) if k > 1 else (0, 1, 3, 4, 6, 7) for k in range(len(pieces))}

    def kernel(dg_ref, du_ref, gu_ref, h_ref, dy_ref, hid_ref, d1_ref, last_ref, dh_ref, od_ref, s_ref, sd_ref, sq_ref, *scratch):
        ad, local = scratch[:2]
        phase, t = place_in_grid()
        place = Place(sizes)
        wide, right = pl.ds(0, WIDE), pl.ds(WIDE, d - WIDE)

        def stored(k):
            own = scratch[2 + k]
            sems = local.at[k]
            return (
                lambda: Stored(place, d1_ref, own, sems, wide),
                lambda: Stored(place, d1_ref, own, sems, right),
                lambda: Stored(place, last_ref, own, sems),
            )[k]()

        def piece(k):
            out = (sd_ref.at[:, :, wide], sd_ref.at[:, :, right], s_ref)[k]
            return Sum(place, *stored(k).terms(), out, sq_ref, parts_of(scratch[2 + len(pieces) :], len(pieces))[k])

        @pl.when(t == 0)
        def _():
            zero(ad, sq_ref)
            for k in plan:
                for one in stored(k).copies():
                    one.start()
            greet(place.around)

        @pl.when(t == 1)
        def _():
            for k in plan:
                for one in stored(k).copies():
                    one.wait()

        scheduled(phase, 1, t, nt, plan, lambda k, stage: piece(k).stages()[stage]())
        for i in range(tb // sub):
            r = pl.ds(i * sub, sub)
            da = dot_nt(gu_ref[0], dg_ref[r, :]).astype(BF16) + dot_nt(gu_ref[1], du_ref[r, :]).astype(BF16)
            da = da.T.astype(F32)
            wide_h = h_ref[r, :].astype(F32)
            scale = rms(wide_h)
            back = scale * da - wide_h * (scale * scale * scale * jnp.mean(da * wide_h, -1, keepdims=True))
            dh_ref[r, :] = dy_ref[r, :] + back.astype(BF16)
        ad[...] += dot(dh_ref[...].T, hid_ref[...])

        @pl.when(t == nt - 1)
        def _():
            transposed(od_ref, ad)
            for k, stage in leftover(plan, nt - 1):
                piece(k).stages()[stage]()
            for k in plan:
                piece(k).sent()

    rows = lambda n: row_blocks(tb, n)
    summed = (2,) + pieces[2]
    scratch = [pltpu.VMEM((d, f), F32), DMA((len(pieces), 4))] + [pltpu.VMEM((4, 2) + p, BF16) for p in pieces]
    for p in pieces:
        scratch += Sum.scratch(sizes["r"], *p)
    return pl.pallas_call(
        kernel,
        grid=(1, nt),
        in_specs=[rows(f), rows(f), fixed(2, d, f), rows(d), rows(d), rows(f), ANY, ANY],
        out_specs=[rows(d), fixed(f, d), fixed(*summed), fixed(2, rows_f, d), fixed(8, LANES)],
        out_shape=[shape(t_, d), shape(f, d), shape(*summed), shape(2, rows_f, d), shape(8, LANES, dtype=F32)],
        scratch_shapes=scratch,
        compiler_params=params(collective_id=2, has_side_effects=True),
        name="middle",
    )(dg, du, gu, h, dy, hid, d1, last)


def backward_bottom(sizes, a, dy, by_gate, by_up, by_gate_n, by_up_n, wd, d0, sq1, sq2, tb=1024, sub=256):
    t_, d = a.shape
    f = wd.shape[0]
    nf, nt = f // WIDE, t_ // tb
    n_s = sizes["s"]
    rows_d, rows_f = d // n_s, f // n_s // 2
    d0 = d0.reshape(2 * n_s, rows_f, d)
    pieces = [(rows_d, WIDE)] * nf + [(rows_d, NARROW), (rows_f, WIDE), (rows_f, d - WIDE)]
    last = (nf + 1) * nt - 1
    slow = (0, 1, 4, 6, 9, 11)
    plan = {nf: after(last + 1, (0, 2, 5, 7, 8, 9)), nf + 1: slow, nf + 2: after(1, slow), 0: after(nt, slow)}
    plan |= {k: after((k + 1) * nt, (0, 1, 3, 5, 8, 10)) for k in range(1, nf)}

    def kernel(a_ref, dy_ref, gate_ref, up_ref, by_gaten_ref, by_upn_ref, wd_ref, d0_ref, sq1_ref, sq2_ref, s_ref, sd_ref, sum_ref, *scratch):
        dgu, acc, own0, own1, terms, terms_n, sq, squares, local, send, recv = scratch[:11]
        phase, t = place_in_grid()
        step = phase * nt + t
        place = Place(sizes)
        wide, right = pl.ds(0, WIDE), pl.ds(WIDE, d - WIDE)
        stored = lambda k: Stored(place, d0_ref, (own0, own1)[k], local.at[k], (wide, right)[k])

        def piece(k):
            part = parts_of(scratch[11:], len(pieces))[k]
            if k > nf:
                return Sum(place, *stored(k - nf - 1).terms(), sd_ref.at[:, :, (wide, right)[k - nf - 1]], sq, part)
            out = s_ref.at[:, :, pl.ds(k * WIDE, pieces[k][1])]
            return Sum(place, *term_blocks(terms.at[k] if k < nf else terms_n, place, rows_d), out, sq, part)

        others = [{"s": lax.rem(place.me + i, n_s)} for i in range(1, n_s)]

        def square_copies():
            return [
                pltpu.make_async_remote_copy(
                    src_ref=sq, dst_ref=squares.at[place.me], send_sem=send.at[i], recv_sem=recv.at[i], device_id=to, device_id_type=MESH
                )
                for i, to in enumerate(others)
            ]

        @pl.when(step == 0)
        def _():
            sq[...] = sq1_ref[...] + sq2_ref[...]
            for k in range(2):
                for one in stored(k).copies():
                    one.start()
            greet(others + [place.up, place.down])
            for k in range(2):
                for one in stored(k).copies():
                    one.wait()

        scheduled(phase, nf + 1, t, nt, plan, lambda k, stage: piece(k).stages()[stage]())

        @pl.when(t == 0)
        def _():
            zero(acc)

        def work(width, gate_ref, up_ref):
            both = pl.ds(0, 2 * width)
            for i in range(tb // sub):
                r = pl.ds(i * sub, sub)
                dh = dot_nt(dy_ref[r, :], wd_ref[pl.ds(0, width), :])
                dh = dh.astype(BF16).astype(F32)
                for one, ref in enumerate((gate_ref, up_ref)):
                    dgu[r, pl.ds(one * width, width)] = (dh * ref[r, :]).astype(BF16)
            acc[:, both] += dot(a_ref[...].T, dgu[:, both])

        @pl.when(phase < nf)
        def _():
            work(WIDE, gate_ref, up_ref)

        @pl.when(phase == nf)
        def _():
            work(NARROW, by_gaten_ref, by_upn_ref)

        @pl.when((t == nt - 1) & (phase < nf))
        def _():
            for i in range(2):
                terms[phase, i] = acc[:, i * WIDE : (i + 1) * WIDE].astype(BF16)

        @pl.when(step == last)
        def _():
            for i in range(2):
                terms_n[i] = acc[:, i * NARROW : (i + 1) * NARROW].astype(BF16)
            for k, stage in leftover(plan, last):
                piece(k).stages()[stage]()
            for one in square_copies():
                one.start()
            squares[place.me] = sq[...]
            for one in square_copies():
                one.wait_recv()
            sum_ref[...] = sum(squares[i] for i in range(n_s))
            for k in range(len(pieces)):
                piece(k).sent()
            for one in square_copies():
                one.wait_send()

    rows = row_blocks(tb, d)
    chunks = block((None, tb, WIDE), lambda p, t: (jnp.minimum(p, nf - 1), jnp.where(p < nf, t, nt - 1), 0))
    narrow = block((tb, NARROW), lambda p, t: (jnp.where(p < nf, 0, t), 0))
    lanes = (8, LANES)
    scratch = [pltpu.VMEM((tb, 2 * WIDE), BF16), pltpu.VMEM((d, 2 * WIDE), F32)]
    scratch += [pltpu.VMEM((4, 2) + p, BF16) for p in pieces[nf + 1 :]]
    scratch += [pltpu.VMEM((nf, 2, d, WIDE), BF16), pltpu.VMEM((2, d, NARROW), BF16), pltpu.VMEM(lanes, F32), pltpu.VMEM((n_s,) + lanes, F32)]
    scratch += [DMA((2, 4)), DMA((n_s - 1,)), DMA((n_s - 1,))]
    for p in pieces:
        scratch += Sum.scratch(sizes["r"], *p)
    return pl.pallas_call(
        kernel,
        grid=(nf + 1, nt),
        in_specs=[rows, rows, chunks, chunks, narrow, narrow, block((WIDE, d), lambda p, t: (p, 0)), ANY, fixed(*lanes), fixed(*lanes)],
        out_specs=[fixed(2, rows_d, f), fixed(2, rows_f, d), fixed(*lanes)],
        out_shape=[shape(2, rows_d, f), shape(2, rows_f, d), shape(*lanes, dtype=F32)],
        scratch_shapes=scratch,
        compiler_params=params(collective_id=3, has_side_effects=True),
        name="backward_bottom",
    )(a, dy, by_gate, by_up, by_gate_n, by_up_n, wd, d0, sq1, sq2)


def update(sizes, weights, m, v, s0, s1, s1_end, sd0, sd1, squares, n=6):
    layers, rows_d, f = weights[0].shape
    rows_f, d = weights[2].shape[1:]
    wide, tall = f // n, rows_f // n
    early = s1.shape[2] // wide
    sd0, sd1 = (one.reshape(rows_f, d) for one in (sd0, sd1))
    count = sizes["s"] * sum(w.size for w in weights)

    def kernel(s0_ref, s1_ref, s1e_ref, sd0_ref, sd1_ref, sq_ref, *refs):
        ins, outs = refs[:9], refs[9:]
        factor = jnp.minimum(1.0, 0.5 * lax.rsqrt(jnp.sum(sq_ref[...], keepdims=True) / count + 1e-30))

        def one(i, layer, g):
            w_ref, m_ref, v_ref = ins[i::3]
            g = g.astype(F32) * factor
            new_m = 0.9 * m_ref[layer] + 0.1 * g
            new_v = 0.95 * v_ref[layer] + 0.05 * g * g
            w = w_ref[layer].astype(F32)
            outs[i][layer] = (w - 0.02 * (new_m * lax.rsqrt(new_v + 1e-8) + 0.1 * w)).astype(BF16)
            outs[i + 3][layer] = new_m
            outs[i + 6][layer] = new_v

        later = [jnp.where(pl.program_id(0) < early, s1_ref[i], s1e_ref[i]) for i in range(2)]
        for layer, (gate, up, down) in enumerate(((*(s0_ref[i] for i in range(2)), sd0_ref[...]), (*later, sd1_ref[...]))):
            for i, g in enumerate((gate, up, down)):
                one(i, layer, g)

    across = lambda first, index: block((first, rows_d, wide), lambda p: (0, 0, index(p)))
    whole = [across(layers, lambda p: p)] * 2 + [block((layers, tall, d), lambda p: (0, p, 0))]
    low = block((tall, d), lambda p: (p, 0))
    arrays = (*weights, *m, *v)
    return pl.pallas_call(
        kernel,
        grid=(n,),
        in_specs=[across(2, lambda p: p), across(2, lambda p: jnp.minimum(p, early - 1)), across(2, lambda p: jnp.maximum(p - early, 0)), low, low, fixed(8, LANES)]
        + whole * 3,
        out_specs=whole * 3,
        out_shape=[jax.ShapeDtypeStruct(one.shape, one.dtype) for one in arrays],
        compiler_params=pltpu.CompilerParams(vmem_limit_bytes=VMEM_LIMIT),
        name="update",
    )(s0, s1, s1_end, sd0, sd1, squares, *arrays)


def solution(mesh):
    sizes = dict(mesh.shape)

    def step(x, dy, *arrays):
        weights, m, v = (arrays[i : i + 3] for i in (0, 3, 6))
        x, dy = x[0], dy[0]
        *slopes, h1, a1, a0, hid, wd0, wd1, gu1 = forward(sizes, x, *weights)
        dg, du, last, d1, s1, sq1 = backward_top(sizes, a1, dy, gu1, wd1)
        dh1, d0, s1_end, sd1, sq2 = middle(sizes, dg, du, gu1, h1, dy, hid, d1, last)
        s0, sd0, squares = backward_bottom(sizes, a0, dh1, *slopes, wd0, d0, sq1, sq2)
        return tuple(update(sizes, weights, m, v, s0, s1, s1_end, sd0, sd1, squares))

    states, cut = P(("rep", "r", "s"), None, None), P(None, "s", None)
    return jax.shard_map(
        step,
        mesh=mesh,
        in_specs=(states, states) + (cut,) * 9,
        out_specs=(P("rep", "s", None),) * 9,
        check_vma=False,
    )
```

```python
import jax
import jax.numpy as jnp
from jax import lax
from jax.experimental import pallas as pl
from jax.experimental.pallas import tpu as pltpu
from jax.sharding import PartitionSpec as P

F32, BF16 = jnp.float32, jnp.bfloat16
MESH = pl.DeviceIdType.MESH
DMA = pltpu.SemaphoreType.DMA
ANY = pl.BlockSpec(memory_space=pl.ANY)
VMEM_LIMIT = 67043328
LANES = 128
WIDE, NARROW = 512, 256


def dot(a, b):
    return jnp.dot(a, b, preferred_element_type=F32)


def dot_nt(a, b):
    return lax.dot_general(a, b, (((1,), (1,)), ((), ())), preferred_element_type=F32)


def params(**more):
    return pltpu.CompilerParams(vmem_limit_bytes=VMEM_LIMIT, dimension_semantics=("arbitrary", "arbitrary"), **more)


def shape(*dims, dtype=BF16):
    return jax.ShapeDtypeStruct(dims, dtype)


def block(dims, index, **more):
    return pl.BlockSpec(dims, index, **more)


def fixed(*dims):
    return pl.BlockSpec(dims, lambda *_: (0,) * len(dims), pipeline_mode=pl.Buffered(1))


def place_in_grid():
    return pl.program_id(0), pl.program_id(1)


def row_blocks(tb, n):
    return block((tb, n), lambda p, t: (t, 0))


def span(i, size, tile=16):
    return pl.ds(pl.multiple_of(i * size, tile), size)


def rms(wide):
    return lax.rsqrt(jnp.mean(wide * wide, -1, keepdims=True) + 1e-6)


def normed(wide):
    return (wide * rms(wide)).astype(BF16)


class Place:
    def __init__(self, sizes):
        self.shards, self.groups = sizes["s"], sizes["r"]
        self.me, self.y = lax.axis_index("s"), lax.axis_index("r")
        self.c = lax.rem(self.me, 2)
        self.right, self.left, self.partner = {"s": self.shard(1)}, {"s": self.shard(-1)}, {"s": self.me + 1 - 2 * self.c}
        self.above, self.below = self.group(1), self.group(-1)
        self.up, self.down = {"r": self.above}, {"r": self.below}
        self.around = [self.left, self.right, self.partner, self.up, self.down]

    def shard(self, chips, other=False):
        s = lax.rem(self.me + 2 * chips + self.shards, self.shards)
        return s + 1 - 2 * self.c if other else s

    def group(self, steps):
        return lax.rem(self.y + steps + self.groups, self.groups)


def greet(devices):
    for device in devices:
        pl.semaphore_signal(pltpu.get_barrier_semaphore(), inc=1, device_id=device, device_id_type=MESH)


def met(devices):
    pl.semaphore_wait(pltpu.get_barrier_semaphore(), len(devices))


class Copies:
    def _copy(self, name, table):
        i = list(table).index(name)
        src, dst, device = table[name]
        return pltpu.make_async_remote_copy(
            src_ref=src, dst_ref=dst, send_sem=self.send.at[i], recv_sem=self.recv.at[i], device_id=device, device_id_type=MESH
        )

    def start(self, *names):
        table = self.table()
        for name in names:
            self._copy(name, table).start()

    def arrived(self, *names):
        table = self.table()
        for name in names:
            self._copy(name, table).wait_recv()

    def sent(self):
        table = self.table()
        for name in table:
            self._copy(name, table).wait_send()


class Gather(Copies):
    N = 17

    def __init__(self, place, own, whole, part, send, recv):
        self.p, self.own, self.whole, self.part, self.send, self.recv = place, own, whole, part, send, recv

    def table(self):
        p, part = self.p, self.part
        have, lack = lax.rem(p.y, 2), 1 - lax.rem(p.y, 2)
        left, right, far = (p.shard(i) for i in (-1, 1, 2))
        mine = part(p.me, have)
        same = lambda device, *which: (part(*which), part(*which), device)
        table = {
            "left": (self.own(have), mine, p.right),
            "right": (self.own(have), mine, p.left),
            "far0": same(p.right, left, have, 0),
            "far1": same(p.left, right, have, 1),
            "up": same(p.up, right, have),
            "down": same(p.down, left, have),
            "far up": same(p.up, far, have, 0),
            "far down": same(p.down, far, have, 1),
            "my own": (self.own(None), self.whole, p.partner),
        }
        for name, *which in (
            ("my left", left, have),
            ("my right", right, have),
            ("my far0", far, have, 0),
            ("my far1", far, have, 1),
            ("my up", right, lack),
            ("my down", left, lack),
            ("my far up", far, lack, 0),
            ("my far down", far, lack, 1),
        ):
            table[name] = same(p.partner, *which)
        return table

    def _pass(self, *chains):
        for first, *rest in chains:
            self.arrived(first)
            self.start(*rest)

    def first(self):
        self.start("left", "right", "my own")

    def relay(self):
        self._pass(("left", "far0", "down", "my left"), ("right", "far1", "up", "my right"))

    def share(self):
        self._pass(("far0", "far up", "my far0"), ("far1", "far down", "my far1"))

    def collect(self):
        self._pass(*((name, "my " + name) for name in ("up", "down", "far up", "far down")))

    def complete(self):
        self.arrived(*(name for name in self.table() if name.startswith("my ")))


def each(rows, one, size=16):
    @pl.loop(0, rows // size)
    def _(i):
        one(span(i, size))


class Sum(Copies):
    N = 14

    @staticmethod
    def scratch(groups, rows, cols):
        return [pltpu.VMEM((n, 2, rows, cols), BF16) for n in (4, 3, 2, 1, groups)] + [DMA((Sum.N,))] * 2

    def __init__(self, place, mine, theirs, out, squares, scratch):
        self.p, self.mine, self.theirs, self.out, self.squares = place, mine, theirs, out, squares
        self.other, sums, got, self.through, self.groups, self.send, self.recv = scratch
        self.rightward, self.leftward, self.farther = (sums.at[i] for i in range(3))
        self.got = [got.at[i] for i in range(2)]

    def table(self):
        p, right, left, far, groups = self.p, self.rightward, self.leftward, self.farther, self.groups
        from_left, from_right = self.got
        through = self.through.at[0]
        mine, below, above = groups.at[p.y], groups.at[p.below, 0], groups.at[p.above, 1]
        table = {i: (self.theirs(i), self.other.at[i], p.partner) for i in range(4)}
        table |= {
            "far0": (far.at[0], through.at[0], p.right),
            "far1": (far.at[1], through.at[1], p.left),
            "near1": (right.at[1], from_left.at[1], p.right),
            "near0": (left.at[0], from_right.at[0], p.left),
            "last0": (right.at[0], from_left.at[0], p.right),
            "last1": (left.at[1], from_right.at[1], p.left),
            "up": (mine, mine, p.up),
            "down": (mine, mine, p.down),
            "relay0": (below, below, p.up),
            "relay1": (above, above, p.down),
        }
        return table

    def _total(self, terms, half, r):
        total = terms[0](half, r).astype(F32)
        for term in terms[1:]:
            total += term(half, r).astype(F32)
        return total.astype(BF16)

    def _own(self, chips):
        return [lambda half, r: self.mine(chips, half, r), lambda half, r: self.other[chips, half, r, :]]

    def _ready(self, dst, terms, half):
        def one(r):
            dst[half, r, :] = self._total(terms, half, r)

        each(dst.shape[1], one)

    def exchange(self):
        self.start(2, 1, 3, 0)

    def far(self):
        self.arrived(2)
        for half in range(2):
            self._ready(self.farther, self._own(2), half)
        self.start("far0", "far1")
        self.arrived(1)
        self._ready(self.rightward, self._own(1), 1)
        self.start("near1")
        self.arrived(3)
        self._ready(self.leftward, self._own(3), 0)
        self.start("near0")

    def near(self):
        through = lambda half, r: self.through[0, half, r, :]
        self.arrived("far0")
        self._ready(self.rightward, self._own(1) + [through], 0)
        self.start("last0")
        self.arrived("far1")
        self._ready(self.leftward, self._own(3) + [through], 1)
        self.start("last1")

    def across(self):
        self.arrived(0, "near1", "near0", "last0", "last1")
        got = [lambda half, r, ref=ref: ref[half, r, :] for ref in self.got]
        for half in range(2):
            self._ready(self.groups.at[self.p.y], self._own(0) + got, half)
        self.start("up", "down")

    def relay(self):
        self.arrived("up")
        self.start("relay0")
        self.arrived("down")
        self.start("relay1")

    def finish(self):
        self.arrived("relay0", "relay1")
        terms = [lambda half, r, i=i: self.groups[i, half, r, :] for i in range(self.groups.shape[0])]
        for half in range(2):

            def one(r):
                g = self._total(terms, half, r)
                self.out[half, r, :] = g
                g = g.astype(F32)
                g = (g * g).reshape(2, -1, g.shape[1])
                g = g[0] + g[1]
                self.squares[...] += sum(g[:, i : i + LANES] for i in range(0, g.shape[1], LANES))

            each(self.out.shape[1], one)

    def stages(self):
        return self.exchange, self.far, self.near, self.across, self.relay, self.finish


def scheduled(phase, phases, t, nt, plan, do, part=0, parts=1):
    table = {}
    for item, steps in plan.items():
        for stage, at in enumerate(steps):
            table.setdefault(at, []).append((item, stage))
    for p in range(phases):
        here = {i: table[at] for i in range(nt) if (at := (p * nt + i) * parts + part) in table}
        if here:

            @pl.when(phase == p)
            def _():
                for i, items in here.items():

                    @pl.when(t == i)
                    def _():
                        for one in items:
                            do(*one)


def leftover(plan, last):
    return [one for _, one in sorted(((at, (k, i)) for k, steps in plan.items() for i, at in enumerate(steps) if at > last), key=lambda one: one[0])]


def after(first, offsets):
    return [first + i for i in offsets]


def columns(first, width):
    def part(ref, rows):
        def one(s, half, q=None):
            start, size = (first, width) if q is None else (first + q * (width // 2), width // 2)
            return ref.at[half, span(s, rows), pl.ds(start, size)]

        return one

    return part


def down_part(ref, rows):
    def one(s, half, q=None):
        cols = {None: pl.ds(0, ref.shape[1]), 0: pl.ds(0, WIDE), 1: pl.ds(WIDE, ref.shape[1] - WIDE)}[q]
        return ref.at[span(2 * s + half, rows // 2), cols]

    return one


def forward(sizes, x, wg, wu, wd, tb=1024, sub=256):
    t_, d = x.shape
    rows_d, f = wg.shape[1:]
    rows_f = wd.shape[1]
    nf, nt = f // WIDE, t_ // tb
    rest = nf * WIDE
    last = (nf + 3) * nt - 1
    plan = dict(
        narrow=(0, 2, 4, 4, nt),
        wide0=(0, 3, 5, 7, 2 * nt),
        wide1=(4, 6, 8, 10, 3 * nt),
        wide2=(6, 11, 13, 15, 4 * nt),
        down0=(9, 13, 15, 18, (nf + 2) * nt),
        down1=(12, 16, 19, 21, last + 1),
        gu1=(14, 20, 24, 26, last + 1),
    )

    def kernel(x_ref, wg_ref, wu_ref, wd_ref, gate_ref, up_ref, gate_n_ref, up_n_ref, h_ref, an_ref, a_ref, hid_ref, wd0_ref, wd1_ref, gu1_ref, *scratch):
        hid_all, a_all, wgu, narrow, wdv, mine_gu, mine_w, local, kept, send, recv = scratch
        phase, t = place_in_grid()
        step = phase * nt + t
        place = Place(sizes)
        mine_d, mine_f = span(place.me, rows_d), span(place.me, rows_f)

        def narrow_part(s, half, q=None):
            start, size = (half * NARROW, NARROW) if q is None else (half * NARROW + q * LANES, LANES)
            return narrow.at[span(s, rows_d), pl.ds(pl.multiple_of(start, LANES), size)]

        def gate_up(k, ref, first, width, own=None):
            part = columns(first, width)(ref, rows_d)
            whole = ref.at[:, mine_d, pl.ds(first, width)]
            if own is None:
                source = lambda half: whole if half is None else part(place.me, half)
            else:
                source = lambda half: own.at[slice(None) if half is None else half, :, pl.ds(first, width)]
            return Gather(place, source, whole, part, send.at[k], recv.at[k])

        def down(k, ref, own=None):
            part, whole = down_part(ref, rows_f), ref.at[mine_f, :]
            if own is None:
                source = lambda half: whole if half is None else part(place.me, half)
            else:
                source = lambda half: own if half is None else own.at[span(half, rows_f // 2), :]
            return Gather(place, source, whole, part, send.at[k], recv.at[k])

        def gather(name):
            k = list(plan).index(name)
            if name == "narrow":
                whole = narrow.at[mine_d, :]
                own = lambda half: whole if half is None else narrow_part(place.me, half)
                return Gather(place, own, whole, narrow_part, send.at[k], recv.at[k])
            return dict(
                wide0=lambda: gate_up(k, wgu, 0, WIDE),
                wide1=lambda: gate_up(k, wgu, WIDE, WIDE),
                wide2=lambda: gate_up(k, wgu, 2 * WIDE, rest - 2 * WIDE),
                down0=lambda: down(k, wdv),
                down1=lambda: down(k, wd1_ref, mine_w),
                gu1=lambda: gate_up(k, gu1_ref, 0, f, mine_gu),
            )[name]()

        def locals_():
            out = []
            for i, ref in enumerate((wg_ref, wu_ref)):
                out.append((ref.at[0, :, pl.ds(rest, NARROW)], narrow.at[mine_d, pl.ds(i * NARROW, NARROW)]))
            for i, ref in enumerate((wg_ref, wu_ref)):
                out.append((ref.at[0, :, pl.ds(0, rest)], wgu.at[i, mine_d, :]))
            out.append((wd_ref.at[0], wdv.at[mine_f, :]))
            out.append((wd_ref.at[1], mine_w))
            for i, ref in enumerate((wg_ref, wu_ref)):
                out.append((ref.at[1], mine_gu.at[i]))
            return [lambda i=i, pair=pair: pltpu.make_async_copy(*pair, local.at[i]) for i, pair in enumerate(out)]

        def keep(k):
            if 0 < k <= nf + 1:
                cols = pl.ds((k - 2) * WIDE, WIDE) if k > 1 else pl.ds(rest, NARROW)
                src, dst = hid_all.at[:, cols], hid_ref.at[:, cols]
            else:
                src, dst = ((a_all, a_ref), (mine_w, wd1_ref.at[mine_f, :]), (mine_gu, gu1_ref.at[:, mine_d, :]), (wdv, wd0_ref))[max(k - nf - 1, 0)]
            return pltpu.make_async_copy(src, dst, kept.at[k])

        @pl.when(step == 0)
        def _():
            for one in locals_():
                one().start()
            greet(place.around)
            for one in locals_()[:5]:
                one().wait()
            met(place.around)

        def stage_of(name, stage):
            if name == "kept":
                keep(stage).start()
                return
            if (name, stage) == ("down1", 0):
                for one in locals_()[5:]:
                    one().wait()
                keep(nf + 2).start()
                keep(nf + 3).start()
            getattr(gather(name), ("first", "relay", "share", "collect", "complete")[stage])()
            if (name, stage) == ("down0", 4):
                keep(nf + 4).start()

        scheduled(phase, nf + 3, t, nt, plan | dict(kept=[(k + 1) * nt for k in range(nf + 2)]), stage_of)
        def save(by_gate_ref, by_up_ref, r, rows, first, gate, up):
            sg = jax.nn.sigmoid(gate)
            si = gate * sg
            by_gate_ref[r, :] = up * (sg + si * (1 - sg))
            by_up_ref[r, :] = si
            hid_all[rows, pl.ds(first, gate.shape[1])] = (si * up).astype(BF16)

        def blocks(one):
            for i in range(tb // sub):
                one(pl.ds(i * sub, sub), span(t * (tb // sub) + i, sub))

        def loop(one):
            size = 2 * sub
            pl.loop(0, tb // size)(lambda i: one(span(i, size), span(t * (tb // size) + i, size)))

        @pl.when(phase == 0)
        def _():
            def one(r, rows):
                a_all[rows, :] = normed(x_ref[r, :].astype(F32))

            blocks(one)

        @pl.when(phase == 1)
        def _():
            def one(r, rows):
                both = dot(a_all[rows, :], narrow[...])
                save(gate_n_ref, up_n_ref, r, rows, rest, both[:, :NARROW], both[:, NARROW:])

            loop(one)

        @pl.when((phase > 1) & (phase < nf + 2))
        def _():
            first = pl.multiple_of((phase - 2) * WIDE, WIDE)

            def one(r, rows):
                for at in range(0, WIDE, NARROW):
                    cols = pl.ds(first + at, NARROW)
                    gate, up = (dot(a_all[rows, :], wgu[i, :, cols]) for i in range(2))
                    save(gate_ref.at[:, pl.ds(at, NARROW)], up_ref.at[:, pl.ds(at, NARROW)], r, rows, first + at, gate, up)

            blocks(one)

        @pl.when(phase == nf + 2)
        def _():
            def one(r, rows):
                h = x_ref[r, :] + dot(hid_all[rows, :], wdv[...]).astype(BF16)
                h_ref[r, :] = h
                an_ref[r, :] = normed(h.astype(F32))

            loop(one)

        @pl.when(step == last)
        def _():
            for k, stage in leftover(plan, last):
                stage_of(k, stage)
            for k in plan:
                gather(k).sent()
            for k in range(nf + 5):
                keep(k).wait()

    def at(p, t, first, final):
        return jnp.where(p < first, 0, jnp.where(p > final, nt - 1, t))

    def during(first, final, width):
        return block((tb, width), lambda p, t: (at(p, t, first, final), 0))

    rows = block((tb, d), lambda p, t: (jnp.where((p > 0) & (p < nf + 2), nt - 1, t), 0))
    wide = block((None, tb, WIDE), lambda p, t: (jnp.clip(p - 2, 0, nf - 1), at(p, t, 2, nf + 1), 0))
    early, late = during(1, 1, NARROW), during(nf + 2, nf + 2, d)
    return pl.pallas_call(
        kernel,
        grid=(nf + 3, nt),
        in_specs=[rows, ANY, ANY, ANY],
        out_specs=[wide, wide, early, early, late, late] + [ANY] * 5,
        out_shape=[shape(nf, t_, WIDE, dtype=F32)] * 2
        + [shape(t_, NARROW, dtype=F32)] * 2
        + [shape(t_, d)] * 3
        + [shape(t_, f), shape(f, d), shape(f, d), shape(2, d, f)],
        scratch_shapes=[
            pltpu.VMEM((t_, f), BF16),
            pltpu.VMEM((t_, d), BF16),
            pltpu.VMEM((2, d, rest), BF16),
            pltpu.VMEM((d, 2 * NARROW), BF16),
            pltpu.VMEM((f, d), BF16),
            pltpu.VMEM((2, rows_d, f), BF16),
            pltpu.VMEM((rows_f, d), BF16),
            DMA((8,)),
            DMA((nf + 5,)),
        ]
        + [DMA((len(plan), Gather.N))] * 2,
        compiler_params=params(collective_id=0, has_side_effects=True),
        name="forward",
    )(x, wg, wu, wd)


def split(gate, up, dh):
    dh = dh.astype(BF16).astype(F32)
    sg = jax.nn.sigmoid(gate)
    si = gate * sg
    return (si * up).astype(BF16), (dh * up * (sg + si * (1 - sg))).astype(BF16), (dh * si).astype(BF16)


def term_blocks(ref, place, rows):
    mine = lambda chips, half, r: ref[half, pl.ds(pl.multiple_of(place.shard(chips) * rows, 16) + r.start, r.size), :]
    return mine, lambda chips: ref.at[:, span(place.shard(chips, True), rows), :]


class Stored:
    def __init__(self, place, ref, own, sems, cols=None):
        self.p, self.ref, self.own, self.sems = place, ref, own, sems
        self.cols = pl.ds(0, ref.shape[-1]) if cols is None else cols

    def block(self, s):
        rows = self.own.shape[2]
        return self.ref.at[pl.ds(2 * s, 2), :, self.cols] if self.ref.shape[0] > 2 else self.ref.at[:, span(s, rows), self.cols]

    def copies(self):
        return [pltpu.make_async_copy(self.block(self.p.shard(i)), self.own.at[i], self.sems.at[i]) for i in range(4)]

    def terms(self):
        return lambda chips, half, r: self.own[chips, half, r, :], lambda chips: self.block(self.p.shard(chips, True))


def parts_of(scratch, count):
    n = len(scratch) // count
    return [scratch[n * k : n * (k + 1)] for k in range(count)]


def accumulate(acc, lhs, rhs, pieces):
    rows = lhs.shape[0] // pieces
    for i in range(pieces):
        r = slice(i * rows, (i + 1) * rows)
        acc[r, :] += dot(lhs[r], rhs[...])


def zero(*refs):
    for ref in refs:
        ref[...] = jnp.zeros_like(ref)


def transposed(dst, src):
    @pl.loop(0, src.shape[1] // LANES)
    def _(i):
        dst[span(i, LANES), :] = src[:, span(i, LANES, LANES)].T.astype(BF16)


def backward_top(sizes, a, dy, gu, wd, nf=3, tb=1024, sub=256):
    t_, d = a.shape
    f = wd.shape[0]
    fc, nt = f // nf, t_ // tb
    rows_d = d // sizes["s"]
    done = nf - 1
    last = nf * nt - 1
    plan = {k: after(2 * (k + 1) * nt, (0, 1, 3, 5, 7, 8)) for k in range(done)}

    def kernel(a_ref, dy_ref, gu_ref, wd_ref, dg_ref, du_ref, last_ref, od_ref, s_ref, sq_ref, *scratch):
        hid, ag, au, ad, terms = scratch[:5]
        phase, t = place_in_grid()
        place = Place(sizes)

        def piece(k):
            out = s_ref.at[:, :, pl.ds(k * fc, fc)]
            return Sum(place, *term_blocks(terms.at[k], place, rows_d), out, sq_ref, parts_of(scratch[5:], done)[k])

        @pl.when(phase * nt + t == 0)
        def _():
            greet(place.around)
            zero(sq_ref)

        def stage_of(k, stage):
            piece(k).stages()[stage]()

        @pl.when((phase == 1) & (t == 0))
        def _():
            met(place.around)

        scheduled(phase, nf, t, nt, plan, stage_of, 0, 2)

        @pl.when(t == 0)
        def _():
            zero(ag, au, ad)

        for i in range(tb // sub):
            r = pl.ds(i * sub, sub)
            av, dv = a_ref[r, :], dy_ref[r, :]
            hid[r, :], dg_ref[r, :], du_ref[r, :] = split(dot(av, gu_ref[0]), dot(av, gu_ref[1]), dot_nt(dv, wd_ref[...]))
        scheduled(phase, nf, t, nt, plan, stage_of, 1, 2)
        accumulate(ad, dy_ref[...].T, hid, 7)
        at = a_ref[...].T
        accumulate(ag, at, dg_ref, 7)
        accumulate(au, at, du_ref, 7)

        def give(ref):
            for i, acc in enumerate((ag, au)):
                ref[i] = acc[...].astype(BF16)

        @pl.when(t == nt - 1)
        def _():
            transposed(od_ref, ad)

        @pl.when((t == nt - 1) & (phase < done))
        def _():
            give(terms.at[phase])

        @pl.when((t == nt - 1) & (phase == done))
        def _():
            give(last_ref)
            for k, stage in leftover(plan, 2 * last + 1):
                stage_of(k, stage)
            for k in range(done):
                piece(k).sent()

    rows = row_blocks(tb, d)
    down = block((fc, d), lambda p, t: (p, 0))
    chunks = block((tb, fc), lambda p, t: (t, p))
    summed = (2, rows_d, done * fc)
    return pl.pallas_call(
        kernel,
        grid=(nf, nt),
        in_specs=[rows, rows, block((2, d, fc), lambda p, t: (0, 0, p)), down],
        out_specs=[chunks, chunks, fixed(2, d, fc), down, fixed(*summed), fixed(8, LANES)],
        out_shape=[shape(t_, f), shape(t_, f), shape(2, d, fc), shape(f, d), shape(*summed), shape(8, LANES, dtype=F32)],
        scratch_shapes=[pltpu.VMEM((tb, fc), BF16)]
        + [pltpu.VMEM((d, fc), F32)] * 3
        + [pltpu.VMEM((done, 2, d, fc), BF16)]
        + Sum.scratch(sizes["r"], rows_d, fc) * done,
        compiler_params=params(collective_id=1, has_side_effects=True),
        name="backward_top",
    )(a, dy, gu, wd)


def middle(sizes, dg, du, gu, h, dy, hid, d1, last, tb=512, sub=256):
    t_, f = dg.shape
    d = h.shape[1]
    nt = t_ // tb
    n_s = sizes["s"]
    rows_d, rows_f = d // n_s, f // n_s // 2
    d1 = d1.reshape(2 * n_s, rows_f, d)
    pieces = [(rows_f, WIDE), (rows_f, d - WIDE), (rows_d, last.shape[2])]
    plan = {k: (2, 4, 9, 11, 14, 2 * nt) if k > 1 else (2, 3, 7, 9, 12, 15) for k in range(len(pieces))}

    def kernel(dg_ref, du_ref, gu_ref, h_ref, dy_ref, hid_ref, d1_ref, last_ref, dh_ref, od_ref, s_ref, sd_ref, sq_ref, *scratch):
        ad, local = scratch[:2]
        phase, t = place_in_grid()
        place = Place(sizes)
        wide, right = pl.ds(0, WIDE), pl.ds(WIDE, d - WIDE)

        def stored(k):
            own = scratch[2 + k]
            sems = local.at[k]
            return (
                lambda: Stored(place, d1_ref, own, sems, wide),
                lambda: Stored(place, d1_ref, own, sems, right),
                lambda: Stored(place, last_ref, own, sems),
            )[k]()

        def piece(k):
            out = (sd_ref.at[:, :, wide], sd_ref.at[:, :, right], s_ref)[k]
            return Sum(place, *stored(k).terms(), out, sq_ref, parts_of(scratch[2 + len(pieces) :], len(pieces))[k])

        @pl.when(t == 0)
        def _():
            zero(ad, sq_ref)
            for k in plan:
                for one in stored(k).copies():
                    one.start()
            greet(place.around)

        @pl.when(t == 1)
        def _():
            for k in plan:
                for one in stored(k).copies():
                    one.wait()
            met(place.around)

        def stage_of(k, stage):
            piece(k).stages()[stage]()

        scheduled(phase, 1, t, nt, plan, stage_of, 0, 2)
        for i in range(tb // sub):
            r = pl.ds(i * sub, sub)
            da = dot_nt(gu_ref[0], dg_ref[r, :]).astype(BF16) + dot_nt(gu_ref[1], du_ref[r, :]).astype(BF16)
            da = da.T.astype(F32)
            wide_h = h_ref[r, :].astype(F32)
            scale = rms(wide_h)
            back = scale * da - wide_h * (scale * scale * scale * jnp.mean(da * wide_h, -1, keepdims=True))
            dh_ref[r, :] = dy_ref[r, :] + back.astype(BF16)
        scheduled(phase, 1, t, nt, plan, stage_of, 1, 2)
        accumulate(ad, dh_ref[...].T, hid_ref, 2)

        @pl.when(t == nt - 1)
        def _():
            transposed(od_ref, ad)
            for k, stage in leftover(plan, 2 * nt - 1):
                stage_of(k, stage)
            for k in plan:
                piece(k).sent()

    rows = lambda n: row_blocks(tb, n)
    summed = (2,) + pieces[2]
    scratch = [pltpu.VMEM((d, f), F32), DMA((len(pieces), 4))] + [pltpu.VMEM((4, 2) + p, BF16) for p in pieces]
    for p in pieces:
        scratch += Sum.scratch(sizes["r"], *p)
    return pl.pallas_call(
        kernel,
        grid=(1, nt),
        in_specs=[rows(f), rows(f), fixed(2, d, f), rows(d), rows(d), rows(f), ANY, ANY],
        out_specs=[rows(d), fixed(f, d), fixed(*summed), fixed(2, rows_f, d), fixed(8, LANES)],
        out_shape=[shape(t_, d), shape(f, d), shape(*summed), shape(2, rows_f, d), shape(8, LANES, dtype=F32)],
        scratch_shapes=scratch,
        compiler_params=params(collective_id=2, has_side_effects=True),
        name="middle",
    )(dg, du, gu, h, dy, hid, d1, last)


def backward_bottom(sizes, a, dy, by_gate, by_up, by_gate_n, by_up_n, wd, d0, sq1, sq2, tb=1024, sub=256):
    t_, d = a.shape
    f = wd.shape[0]
    nf, nt = f // WIDE, t_ // tb
    n_s = sizes["s"]
    rows_d, rows_f = d // n_s, f // n_s // 2
    d0 = d0.reshape(2 * n_s, rows_f, d)
    pieces = [(rows_d, WIDE)] * nf + [(rows_d, NARROW), (rows_f, WIDE), (rows_f, d - WIDE)]
    last = (nf + 1) * nt - 1
    slow = (0, 1, 4, 6, 9, 11)
    plan = {nf: after(last + 1, (0, 2, 5, 7, 8, 9)), nf + 1: after(1, slow), nf + 2: after(2, slow), 0: after(nt, slow)}
    plan |= {k: after((k + 1) * nt, (0, 1, 3, 5, 8, 10)) for k in range(1, nf)}

    def kernel(a_ref, dy_ref, gate_ref, up_ref, by_gaten_ref, by_upn_ref, wd_ref, d0_ref, sq1_ref, sq2_ref, s_ref, sd_ref, sum_ref, *scratch):
        dgu, acc, own0, own1, terms, terms_n, sq, squares, local, send, recv = scratch[:11]
        phase, t = place_in_grid()
        step = phase * nt + t
        place = Place(sizes)
        wide, right = pl.ds(0, WIDE), pl.ds(WIDE, d - WIDE)
        stored = lambda k: Stored(place, d0_ref, (own0, own1)[k], local.at[k], (wide, right)[k])

        def piece(k):
            part = parts_of(scratch[11:], len(pieces))[k]
            if k > nf:
                return Sum(place, *stored(k - nf - 1).terms(), sd_ref.at[:, :, (wide, right)[k - nf - 1]], sq, part)
            out = s_ref.at[:, :, pl.ds(k * WIDE, pieces[k][1])]
            return Sum(place, *term_blocks(terms.at[k] if k < nf else terms_n, place, rows_d), out, sq, part)

        others = [{"s": lax.rem(place.me + i, n_s)} for i in range(1, n_s)]

        def square_copies():
            return [
                pltpu.make_async_remote_copy(
                    src_ref=sq, dst_ref=squares.at[place.me], send_sem=send.at[i], recv_sem=recv.at[i], device_id=to, device_id_type=MESH
                )
                for i, to in enumerate(others)
            ]

        @pl.when(step == 0)
        def _():
            sq[...] = sq1_ref[...] + sq2_ref[...]
            for k in range(2):
                for one in stored(k).copies():
                    one.start()
            greet(others + [place.up, place.down])

        @pl.when(step == 1)
        def _():
            for k in range(2):
                for one in stored(k).copies():
                    one.wait()
            met(others + [place.up, place.down])

        scheduled(phase, nf + 1, t, nt, plan, lambda k, stage: piece(k).stages()[stage]())

        @pl.when(t == 0)
        def _():
            zero(acc)

        def work(width, gate_ref, up_ref):
            both = pl.ds(0, 2 * width)
            for i in range(tb // sub):
                r = pl.ds(i * sub, sub)
                dh = dot_nt(dy_ref[r, :], wd_ref[pl.ds(0, width), :])
                dh = dh.astype(BF16).astype(F32)
                for one, ref in enumerate((gate_ref, up_ref)):
                    dgu[r, pl.ds(one * width, width)] = (dh * ref[r, :]).astype(BF16)
            acc[:, both] += dot(a_ref[...].T, dgu[:, both])

        @pl.when(phase < nf)
        def _():
            work(WIDE, gate_ref, up_ref)

        @pl.when(phase == nf)
        def _():
            work(NARROW, by_gaten_ref, by_upn_ref)

        @pl.when((t == nt - 1) & (phase < nf))
        def _():
            for i in range(2):
                terms[phase, i] = acc[:, i * WIDE : (i + 1) * WIDE].astype(BF16)

        @pl.when(step == last)
        def _():
            for i in range(2):
                terms_n[i] = acc[:, i * NARROW : (i + 1) * NARROW].astype(BF16)
            for k, stage in leftover(plan, last):
                piece(k).stages()[stage]()
            for one in square_copies():
                one.start()
            squares[place.me] = sq[...]
            for one in square_copies():
                one.wait_recv()
            sum_ref[...] = sum(squares[i] for i in range(n_s))
            for k in range(len(pieces)):
                piece(k).sent()
            for one in square_copies():
                one.wait_send()

    rows = row_blocks(tb, d)
    chunks = block((None, tb, WIDE), lambda p, t: (jnp.minimum(p, nf - 1), jnp.where(p < nf, t, nt - 1), 0))
    narrow = block((tb, NARROW), lambda p, t: (jnp.where(p < nf, 0, t), 0))
    lanes = (8, LANES)
    scratch = [pltpu.VMEM((tb, 2 * WIDE), BF16), pltpu.VMEM((d, 2 * WIDE), F32)]
    scratch += [pltpu.VMEM((4, 2) + p, BF16) for p in pieces[nf + 1 :]]
    scratch += [pltpu.VMEM((nf, 2, d, WIDE), BF16), pltpu.VMEM((2, d, NARROW), BF16), pltpu.VMEM(lanes, F32), pltpu.VMEM((n_s,) + lanes, F32)]
    scratch += [DMA((2, 4)), DMA((n_s - 1,)), DMA((n_s - 1,))]
    for p in pieces:
        scratch += Sum.scratch(sizes["r"], *p)
    return pl.pallas_call(
        kernel,
        grid=(nf + 1, nt),
        in_specs=[rows, rows, chunks, chunks, narrow, narrow, block((WIDE, d), lambda p, t: (p, 0)), ANY, fixed(*lanes), fixed(*lanes)],
        out_specs=[fixed(2, rows_d, f), fixed(2, rows_f, d), fixed(*lanes)],
        out_shape=[shape(2, rows_d, f), shape(2, rows_f, d), shape(*lanes, dtype=F32)],
        scratch_shapes=scratch,
        compiler_params=params(collective_id=3, has_side_effects=True),
        name="backward_bottom",
    )(a, dy, by_gate, by_up, by_gate_n, by_up_n, wd, d0, sq1, sq2)


def update(sizes, weights, m, v, s0, s1, s1_end, sd0, sd1, squares):
    layers = weights[0].shape[0]
    sd0, sd1 = (one.reshape(weights[2].shape[1:]) for one in (sd0, sd1))
    count = sizes["s"] * sum(w.size for w in weights)
    early = s1.shape[2]
    arrays = (*weights, *m, *v)
    n = len(arrays)
    kinds = len(weights)

    def kernel(s0_ref, s1_ref, s1e_ref, sd0_ref, sd1_ref, sq_ref, *refs):
        ins, outs, held, (arrive, leave) = refs[:n], refs[n : 2 * n], refs[2 * n : 3 * n], refs[3 * n :]
        order = [(i, layer) for layer in range(layers) for i in range(kinds)]

        def copies(i, layer, back=False):
            out = []
            for k in range(i, n, kinds):
                src, dst, sem = (held[k], outs[k], leave) if back else (ins[k], held[k], arrive)
                out.append(pltpu.make_async_copy(src.at[layer], dst.at[layer], sem.at[k, layer]))
            return out

        for i, layer in order:
            for one in copies(i, layer):
                one.start()
        factor = jnp.minimum(1.0, 0.5 * lax.rsqrt(jnp.sum(sq_ref[...], keepdims=True) / count + 1e-30))
        for i, layer in order:
            for one in copies(i, layer):
                one.wait()
            w_ref, m_ref, v_ref = held[i::kinds]

            def change(g, cols, r):
                g = g[r, :].astype(F32) * factor
                new_m = 0.9 * m_ref[layer, r, cols] + 0.1 * g
                new_v = 0.95 * v_ref[layer, r, cols] + 0.05 * g * g
                w = w_ref[layer, r, cols].astype(F32)
                w_ref[layer, r, cols] = (w - 0.02 * (new_m * lax.rsqrt(new_v + 1e-8) + 0.1 * w)).astype(BF16)
                m_ref[layer, r, cols] = new_m
                v_ref[layer, r, cols] = new_v

            rows, width = w_ref.shape[1:]
            if i == kinds - 1:
                parts = [((sd0_ref, sd1_ref)[layer], pl.ds(0, width))]
            elif layer == 0:
                parts = [(s0_ref.at[i], pl.ds(0, width))]
            else:
                parts = [(s1_ref.at[i], pl.ds(0, early)), (s1e_ref.at[i], pl.ds(early, width - early))]
            for g, cols in parts:
                each(rows, lambda r, g=g, cols=cols: change(g, cols, r))
            for one in copies(i, layer, True):
                one.start()
        for i, layer in order:
            for one in copies(i, layer, True):
                one.wait()

    sums = (s0, s1, s1_end, sd0, sd1, squares)
    return pl.pallas_call(
        kernel,
        in_specs=[pl.BlockSpec(memory_space=pltpu.VMEM)] * len(sums) + [ANY] * n,
        out_specs=[ANY] * n,
        out_shape=[jax.ShapeDtypeStruct(one.shape, one.dtype) for one in arrays],
        scratch_shapes=[pltpu.VMEM(one.shape, one.dtype) for one in arrays] + [DMA((n, layers))] * 2,
        compiler_params=pltpu.CompilerParams(vmem_limit_bytes=VMEM_LIMIT),
        name="update",
    )(*sums, *arrays)


def solution(mesh):
    sizes = dict(mesh.shape)

    def step(x, dy, *arrays):
        weights, m, v = (arrays[i : i + 3] for i in (0, 3, 6))
        x, dy = x[0], dy[0]
        *slopes, h1, a1, a0, hid, wd0, wd1, gu1 = forward(sizes, x, *weights)
        dg, du, last, d1, s1, sq1 = backward_top(sizes, a1, dy, gu1, wd1)
        dh1, d0, s1_end, sd1, sq2 = middle(sizes, dg, du, gu1, h1, dy, hid, d1, last)
        s0, sd0, squares = backward_bottom(sizes, a0, dh1, *slopes, wd0, d0, sq1, sq2)
        return tuple(update(sizes, weights, m, v, s0, s1, s1_end, sd0, sd1, squares))

    states, cut = P(("rep", "r", "s"), None, None), P(None, "s", None)
    return jax.shard_map(
        step,
        mesh=mesh,
        in_specs=(states, states) + (cut,) * 9,
        out_specs=(P("rep", "s", None),) * 9,
        check_vma=False,
    )
```

```python
import jax
import jax.numpy as jnp
from jax import lax
from jax.experimental import pallas as pl
from jax.experimental.pallas import tpu as pltpu
from jax.sharding import PartitionSpec as P

F32, BF16 = jnp.float32, jnp.bfloat16
MESH = pl.DeviceIdType.MESH
DMA = pltpu.SemaphoreType.DMA
ANY = pl.BlockSpec(memory_space=pl.ANY)
VMEM_LIMIT = 67043328
LANES = 128
WIDE, NARROW = 512, 256


def dot(a, b):
    return jnp.dot(a, b, preferred_element_type=F32)


def dot_nt(a, b):
    return lax.dot_general(a, b, (((1,), (1,)), ((), ())), preferred_element_type=F32)


def params(**more):
    return pltpu.CompilerParams(vmem_limit_bytes=VMEM_LIMIT, dimension_semantics=("arbitrary", "arbitrary"), **more)


def shape(*dims, dtype=BF16):
    return jax.ShapeDtypeStruct(dims, dtype)


def block(dims, index, **more):
    return pl.BlockSpec(dims, index, **more)


def fixed(*dims):
    return pl.BlockSpec(dims, lambda *_: (0,) * len(dims), pipeline_mode=pl.Buffered(1))


def place_in_grid():
    return pl.program_id(0), pl.program_id(1)


def row_blocks(tb, n):
    return block((tb, n), lambda p, t: (t, 0))


def span(i, size, tile=16):
    return pl.ds(pl.multiple_of(i * size, tile), size)


def rms(wide):
    return lax.rsqrt(jnp.mean(wide * wide, -1, keepdims=True) + 1e-6)


def normed(wide):
    return (wide * rms(wide)).astype(BF16)


class Place:
    def __init__(self, sizes):
        self.shards, self.groups = sizes["s"], sizes["r"]
        self.me, self.y = lax.axis_index("s"), lax.axis_index("r")
        self.c = lax.rem(self.me, 2)
        self.right, self.left, self.partner = {"s": self.shard(1)}, {"s": self.shard(-1)}, {"s": self.me + 1 - 2 * self.c}
        self.above, self.below = self.group(1), self.group(-1)
        self.up, self.down = {"r": self.above}, {"r": self.below}
        self.around = [self.left, self.right, self.partner, self.up, self.down]

    def shard(self, chips, other=False):
        s = lax.rem(self.me + 2 * chips + self.shards, self.shards)
        return s + 1 - 2 * self.c if other else s

    def group(self, steps):
        return lax.rem(self.y + steps + self.groups, self.groups)


def greet(devices):
    for device in devices:
        pl.semaphore_signal(pltpu.get_barrier_semaphore(), inc=1, device_id=device, device_id_type=MESH)


def met(devices):
    pl.semaphore_wait(pltpu.get_barrier_semaphore(), len(devices))


class Copies:
    def _copy(self, name, table):
        i = list(table).index(name)
        src, dst, device = table[name]
        return pltpu.make_async_remote_copy(
            src_ref=src, dst_ref=dst, send_sem=self.send.at[i], recv_sem=self.recv.at[i], device_id=device, device_id_type=MESH
        )

    def start(self, *names):
        table = self.table()
        for name in names:
            self._copy(name, table).start()

    def arrived(self, *names):
        table = self.table()
        for name in names:
            self._copy(name, table).wait_recv()

    def sent(self):
        table = self.table()
        for name in table:
            self._copy(name, table).wait_send()


class Gather(Copies):
    N = 17

    def __init__(self, place, own, whole, part, send, recv):
        self.p, self.own, self.whole, self.part, self.send, self.recv = place, own, whole, part, send, recv

    def table(self):
        p, part = self.p, self.part
        have, lack = lax.rem(p.y, 2), 1 - lax.rem(p.y, 2)
        left, right, far = (p.shard(i) for i in (-1, 1, 2))
        mine = part(p.me, have)
        same = lambda device, *which: (part(*which), part(*which), device)
        table = {
            "left": (self.own(have), mine, p.right),
            "right": (self.own(have), mine, p.left),
            "far0": same(p.right, left, have, 0),
            "far1": same(p.left, right, have, 1),
            "up": same(p.up, right, have),
            "down": same(p.down, left, have),
            "far up": same(p.up, far, have, 0),
            "far down": same(p.down, far, have, 1),
            "my own": (self.own(None), self.whole, p.partner),
        }
        for name, *which in (
            ("my left", left, have),
            ("my right", right, have),
            ("my far0", far, have, 0),
            ("my far1", far, have, 1),
            ("my up", right, lack),
            ("my down", left, lack),
            ("my far up", far, lack, 0),
            ("my far down", far, lack, 1),
        ):
            table[name] = same(p.partner, *which)
        return table

    def _pass(self, *chains):
        for first, *rest in chains:
            self.arrived(first)
            self.start(*rest)

    def first(self):
        self.start("left", "right", "my own")

    def relay(self):
        self._pass(("left", "far0", "down", "my left"), ("right", "far1", "up", "my right"))

    def share(self):
        self._pass(("far0", "far up", "my far0"), ("far1", "far down", "my far1"))

    def collect(self):
        self._pass(*((name, "my " + name) for name in ("up", "down", "far up", "far down")))

    def complete(self):
        self.arrived(*(name for name in self.table() if name.startswith("my ")))


def each(rows, one, size=16):
    @pl.loop(0, rows // size)
    def _(i):
        one(span(i, size))


class Sum(Copies):
    N = 14

    @staticmethod
    def scratch(groups, rows, cols):
        return [pltpu.VMEM((n, 2, rows, cols), BF16) for n in (4, 3, 2, 1, groups)] + [DMA((Sum.N,))] * 2

    def __init__(self, place, mine, theirs, out, squares, scratch):
        self.p, self.mine, self.theirs, self.out, self.squares = place, mine, theirs, out, squares
        self.other, sums, got, self.through, self.groups, self.send, self.recv = scratch
        self.rightward, self.leftward, self.farther = (sums.at[i] for i in range(3))
        self.got = [got.at[i] for i in range(2)]

    def table(self):
        p, right, left, far, groups = self.p, self.rightward, self.leftward, self.farther, self.groups
        from_left, from_right = self.got
        through = self.through.at[0]
        mine, below, above = groups.at[p.y], groups.at[p.below, 0], groups.at[p.above, 1]
        table = {i: (self.theirs(i), self.other.at[i], p.partner) for i in range(4)}
        table |= {
            "far0": (far.at[0], through.at[0], p.right),
            "far1": (far.at[1], through.at[1], p.left),
            "near1": (right.at[1], from_left.at[1], p.right),
            "near0": (left.at[0], from_right.at[0], p.left),
            "last0": (right.at[0], from_left.at[0], p.right),
            "last1": (left.at[1], from_right.at[1], p.left),
            "up": (mine, mine, p.up),
            "down": (mine, mine, p.down),
            "relay0": (below, below, p.up),
            "relay1": (above, above, p.down),
        }
        return table

    def _total(self, terms, half, r):
        total = terms[0](half, r).astype(F32)
        for term in terms[1:]:
            total += term(half, r).astype(F32)
        return total.astype(BF16)

    def _own(self, chips):
        return [lambda half, r: self.mine(chips, half, r), lambda half, r: self.other[chips, half, r, :]]

    def _ready(self, dst, terms, half):
        def one(r):
            dst[half, r, :] = self._total(terms, half, r)

        each(dst.shape[1], one)

    def exchange(self):
        self.start(2, 1, 3, 0)

    def far(self):
        self.arrived(2)
        for half in range(2):
            self._ready(self.farther, self._own(2), half)
        self.start("far0", "far1")
        self.arrived(1)
        self._ready(self.rightward, self._own(1), 1)
        self.start("near1")
        self.arrived(3)
        self._ready(self.leftward, self._own(3), 0)
        self.start("near0")

    def near(self):
        through = lambda half, r: self.through[0, half, r, :]
        self.arrived("far0")
        self._ready(self.rightward, self._own(1) + [through], 0)
        self.start("last0")
        self.arrived("far1")
        self._ready(self.leftward, self._own(3) + [through], 1)
        self.start("last1")

    def across(self):
        self.arrived(0, "near1", "near0", "last0", "last1")
        got = [lambda half, r, ref=ref: ref[half, r, :] for ref in self.got]
        for half in range(2):
            self._ready(self.groups.at[self.p.y], self._own(0) + got, half)
        self.start("up", "down")

    def relay(self):
        self.arrived("up")
        self.start("relay0")
        self.arrived("down")
        self.start("relay1")

    def finish(self):
        self.arrived("relay0", "relay1")
        terms = [lambda half, r, i=i: self.groups[i, half, r, :] for i in range(self.groups.shape[0])]
        for half in range(2):

            def one(r):
                g = self._total(terms, half, r)
                self.out[half, r, :] = g
                g = g.astype(F32)
                g = (g * g).reshape(2, -1, g.shape[1])
                g = g[0] + g[1]
                self.squares[...] += sum(g[:, i : i + LANES] for i in range(0, g.shape[1], LANES))

            each(self.out.shape[1], one)

    def stages(self):
        return self.exchange, self.far, self.near, self.across, self.relay, self.finish


def scheduled(phase, phases, t, nt, plan, do, part=0, parts=1):
    table = {}
    for item, steps in plan.items():
        for stage, at in enumerate(steps):
            table.setdefault(at, []).append((item, stage))
    for p in range(phases):
        here = {i: table[at] for i in range(nt) if (at := (p * nt + i) * parts + part) in table}
        if here:

            @pl.when(phase == p)
            def _():
                for i, items in here.items():

                    @pl.when(t == i)
                    def _():
                        for one in items:
                            do(*one)


def leftover(plan, last):
    return [one for _, one in sorted(((at, (k, i)) for k, steps in plan.items() for i, at in enumerate(steps) if at > last), key=lambda one: one[0])]


def after(first, offsets):
    return [first + i for i in offsets]


def columns(first, width):
    def part(ref, rows):
        def one(s, half, q=None):
            start, size = (first, width) if q is None else (first + q * (width // 2), width // 2)
            return ref.at[half, span(s, rows), pl.ds(start, size)]

        return one

    return part


def down_part(ref, rows):
    def one(s, half, q=None):
        cols = {None: pl.ds(0, ref.shape[1]), 0: pl.ds(0, WIDE), 1: pl.ds(WIDE, ref.shape[1] - WIDE)}[q]
        return ref.at[span(2 * s + half, rows // 2), cols]

    return one


def forward(sizes, x, wg, wu, wd, tb=1024, sub=256):
    t_, d = x.shape
    rows_d, f = wg.shape[1:]
    rows_f = wd.shape[1]
    nf, nt = f // WIDE, t_ // tb
    rest = nf * WIDE
    last = (nf + 3) * nt - 1
    plan = dict(
        narrow=(0, 2, 4, 4, nt),
        wide0=(0, 3, 4, 6, 2 * nt),
        wide1=(4, 6, 8, 10, 3 * nt),
        wide2=(6, 11, 13, 15, 4 * nt),
        down0=(9, 13, 15, 18, (nf + 2) * nt),
        down1=(12, 16, 19, 21, last + 1),
        gu1=(14, 20, 24, 26, last + 1),
    )

    def kernel(x_ref, wg_ref, wu_ref, wd_ref, gate_ref, up_ref, gate_n_ref, up_n_ref, h_ref, an_ref, a_ref, hid_ref, wd0_ref, wd1_ref, gu1_ref, *scratch):
        hid_all, a_all, wgu, narrow, wdv, mine_gu, mine_w, local, kept, send, recv = scratch
        phase, t = place_in_grid()
        step = phase * nt + t
        place = Place(sizes)
        mine_d, mine_f = span(place.me, rows_d), span(place.me, rows_f)

        def narrow_part(s, half, q=None):
            start, size = (half * NARROW, NARROW) if q is None else (half * NARROW + q * LANES, LANES)
            return narrow.at[span(s, rows_d), pl.ds(pl.multiple_of(start, LANES), size)]

        def gate_up(k, ref, first, width, own=None):
            part = columns(first, width)(ref, rows_d)
            whole = ref.at[:, mine_d, pl.ds(first, width)]
            if own is None:
                source = lambda half: whole if half is None else part(place.me, half)
            else:
                source = lambda half: own.at[slice(None) if half is None else half, :, pl.ds(first, width)]
            return Gather(place, source, whole, part, send.at[k], recv.at[k])

        def down(k, ref, own=None):
            part, whole = down_part(ref, rows_f), ref.at[mine_f, :]
            if own is None:
                source = lambda half: whole if half is None else part(place.me, half)
            else:
                source = lambda half: own if half is None else own.at[span(half, rows_f // 2), :]
            return Gather(place, source, whole, part, send.at[k], recv.at[k])

        def gather(name):
            k = list(plan).index(name)
            if name == "narrow":
                whole = narrow.at[mine_d, :]
                own = lambda half: whole if half is None else narrow_part(place.me, half)
                return Gather(place, own, whole, narrow_part, send.at[k], recv.at[k])
            return dict(
                wide0=lambda: gate_up(k, wgu, 0, WIDE),
                wide1=lambda: gate_up(k, wgu, WIDE, WIDE),
                wide2=lambda: gate_up(k, wgu, 2 * WIDE, rest - 2 * WIDE),
                down0=lambda: down(k, wdv),
                down1=lambda: down(k, wd1_ref, mine_w),
                gu1=lambda: gate_up(k, gu1_ref, 0, f, mine_gu),
            )[name]()

        def locals_():
            out = []
            for i, ref in enumerate((wg_ref, wu_ref)):
                out.append((ref.at[0, :, pl.ds(rest, NARROW)], narrow.at[mine_d, pl.ds(i * NARROW, NARROW)]))
            for i, ref in enumerate((wg_ref, wu_ref)):
                out.append((ref.at[0, :, pl.ds(0, rest)], wgu.at[i, mine_d, :]))
            out.append((wd_ref.at[0], wdv.at[mine_f, :]))
            out.append((wd_ref.at[1], mine_w))
            for i, ref in enumerate((wg_ref, wu_ref)):
                out.append((ref.at[1], mine_gu.at[i]))
            return [lambda i=i, pair=pair: pltpu.make_async_copy(*pair, local.at[i]) for i, pair in enumerate(out)]

        def keep(k):
            if 0 < k <= nf + 1:
                cols = pl.ds((k - 2) * WIDE, WIDE) if k > 1 else pl.ds(rest, NARROW)
                src, dst = hid_all.at[:, cols], hid_ref.at[:, cols]
            else:
                src, dst = ((a_all, a_ref), (mine_w, wd1_ref.at[mine_f, :]), (mine_gu, gu1_ref.at[:, mine_d, :]), (wdv, wd0_ref))[max(k - nf - 1, 0)]
            return pltpu.make_async_copy(src, dst, kept.at[k])

        @pl.when(step == 0)
        def _():
            greet(place.around)
            for one in locals_():
                one().start()
            for one in locals_()[:2]:
                one().wait()
            met(place.around)

        def stage_of(name, stage):
            if name == "kept":
                keep(stage).start()
                return
            if (name, stage) == ("wide0", 0):
                for one in locals_()[2:5]:
                    one().wait()
            if (name, stage) == ("down1", 0):
                for one in locals_()[5:]:
                    one().wait()
                keep(nf + 2).start()
                keep(nf + 3).start()
            getattr(gather(name), ("first", "relay", "share", "collect", "complete")[stage])()
            if (name, stage) == ("down0", 4):
                keep(nf + 4).start()

        scheduled(phase, nf + 3, t, nt, plan | dict(kept=[(k + 1) * nt for k in range(nf + 2)]), stage_of)
        def save(by_gate_ref, by_up_ref, r, rows, first, gate, up):
            sg = jax.nn.sigmoid(gate)
            si = gate * sg
            by_gate_ref[r, :] = up * (sg + si * (1 - sg))
            by_up_ref[r, :] = si
            hid_all[rows, pl.ds(first, gate.shape[1])] = (si * up).astype(BF16)

        def blocks(one):
            for i in range(tb // sub):
                one(pl.ds(i * sub, sub), span(t * (tb // sub) + i, sub))

        def loop(one):
            size = 2 * sub
            pl.loop(0, tb // size)(lambda i: one(span(i, size), span(t * (tb // size) + i, size)))

        @pl.when(phase == 0)
        def _():
            def one(r, rows):
                a_all[rows, :] = normed(x_ref[r, :].astype(F32))

            blocks(one)

        @pl.when(phase == 1)
        def _():
            def one(r, rows):
                both = dot(a_all[rows, :], narrow[...])
                save(gate_n_ref, up_n_ref, r, rows, rest, both[:, :NARROW], both[:, NARROW:])

            loop(one)

        @pl.when((phase > 1) & (phase < nf + 2))
        def _():
            first = pl.multiple_of((phase - 2) * WIDE, WIDE)

            def one(r, rows):
                for at in range(0, WIDE, NARROW):
                    cols = pl.ds(first + at, NARROW)
                    gate, up = (dot(a_all[rows, :], wgu[i, :, cols]) for i in range(2))
                    save(gate_ref.at[:, pl.ds(at, NARROW)], up_ref.at[:, pl.ds(at, NARROW)], r, rows, first + at, gate, up)

            blocks(one)

        @pl.when(phase == nf + 2)
        def _():
            def one(r, rows):
                h = x_ref[r, :] + dot(hid_all[rows, :], wdv[...]).astype(BF16)
                h_ref[r, :] = h
                an_ref[r, :] = normed(h.astype(F32))

            loop(one)

        @pl.when(step == last)
        def _():
            for k, stage in leftover(plan, last):
                stage_of(k, stage)
            for k in plan:
                gather(k).sent()
            for k in range(nf + 5):
                keep(k).wait()

    def at(p, t, first, final):
        return jnp.where(p < first, 0, jnp.where(p > final, nt - 1, t))

    def during(first, final, width):
        return block((tb, width), lambda p, t: (at(p, t, first, final), 0))

    rows = block((tb, d), lambda p, t: (jnp.where((p > 0) & (p < nf + 2), nt - 1, t), 0))
    wide = block((None, tb, WIDE), lambda p, t: (jnp.clip(p - 2, 0, nf - 1), at(p, t, 2, nf + 1), 0))
    early, late = during(1, 1, NARROW), during(nf + 2, nf + 2, d)
    return pl.pallas_call(
        kernel,
        grid=(nf + 3, nt),
        in_specs=[rows, ANY, ANY, ANY],
        out_specs=[wide, wide, early, early, late, late] + [ANY] * 5,
        out_shape=[shape(nf, t_, WIDE, dtype=F32)] * 2
        + [shape(t_, NARROW, dtype=F32)] * 2
        + [shape(t_, d)] * 3
        + [shape(t_, f), shape(f, d), shape(f, d), shape(2, d, f)],
        scratch_shapes=[
            pltpu.VMEM((t_, f), BF16),
            pltpu.VMEM((t_, d), BF16),
            pltpu.VMEM((2, d, rest), BF16),
            pltpu.VMEM((d, 2 * NARROW), BF16),
            pltpu.VMEM((f, d), BF16),
            pltpu.VMEM((2, rows_d, f), BF16),
            pltpu.VMEM((rows_f, d), BF16),
            DMA((8,)),
            DMA((nf + 5,)),
        ]
        + [DMA((len(plan), Gather.N))] * 2,
        compiler_params=params(collective_id=0, has_side_effects=True),
        name="forward",
    )(x, wg, wu, wd)


def split(gate, up, dh):
    dh = dh.astype(BF16).astype(F32)
    sg = jax.nn.sigmoid(gate)
    si = gate * sg
    return (si * up).astype(BF16), (dh * up * (sg + si * (1 - sg))).astype(BF16), (dh * si).astype(BF16)


def term_blocks(ref, place, rows):
    mine = lambda chips, half, r: ref[half, pl.ds(pl.multiple_of(place.shard(chips) * rows, 16) + r.start, r.size), :]
    return mine, lambda chips: ref.at[:, span(place.shard(chips, True), rows), :]


class Stored:
    def __init__(self, place, ref, own, sems, cols=None):
        self.p, self.ref, self.own, self.sems = place, ref, own, sems
        self.cols = pl.ds(0, ref.shape[-1]) if cols is None else cols

    def block(self, s):
        rows = self.own.shape[2]
        return self.ref.at[pl.ds(2 * s, 2), :, self.cols] if self.ref.shape[0] > 2 else self.ref.at[:, span(s, rows), self.cols]

    def copies(self):
        return [pltpu.make_async_copy(self.block(self.p.shard(i)), self.own.at[i], self.sems.at[i]) for i in range(4)]

    def terms(self):
        return lambda chips, half, r: self.own[chips, half, r, :], lambda chips: self.block(self.p.shard(chips, True))


def parts_of(scratch, count):
    n = len(scratch) // count
    return [scratch[n * k : n * (k + 1)] for k in range(count)]


def accumulate(acc, lhs, rhs, pieces):
    rows = lhs.shape[0] // pieces
    for i in range(pieces):
        r = slice(i * rows, (i + 1) * rows)
        acc[r, :] += dot(lhs[r], rhs[...])


def zero(*refs):
    for ref in refs:
        ref[...] = jnp.zeros_like(ref)


def transposed(dst, src):
    @pl.loop(0, src.shape[1] // LANES)
    def _(i):
        dst[span(i, LANES), :] = src[:, span(i, LANES, LANES)].T.astype(BF16)


def backward_top(sizes, a, dy, gu, wd, nf=3, tb=1024, sub=256):
    t_, d = a.shape
    f = wd.shape[0]
    fc, nt = f // nf, t_ // tb
    rows_d = d // sizes["s"]
    done = nf - 1
    last = nf * nt - 1
    plan = {k: after(2 * (k + 1) * nt, (0, 1, 3, 5, 7, 8)) for k in range(done)}

    def kernel(a_ref, dy_ref, gu_ref, wd_ref, dg_ref, du_ref, last_ref, od_ref, s_ref, sq_ref, *scratch):
        hid, ag, au, ad, terms = scratch[:5]
        phase, t = place_in_grid()
        place = Place(sizes)

        def piece(k):
            out = s_ref.at[:, :, pl.ds(k * fc, fc)]
            return Sum(place, *term_blocks(terms.at[k], place, rows_d), out, sq_ref, parts_of(scratch[5:], done)[k])

        @pl.when(phase * nt + t == 0)
        def _():
            greet(place.around)
            zero(sq_ref)

        def stage_of(k, stage):
            piece(k).stages()[stage]()

        @pl.when((phase == 1) & (t == 0))
        def _():
            met(place.around)

        scheduled(phase, nf, t, nt, plan, stage_of, 0, 2)

        @pl.when(t == 0)
        def _():
            zero(ag, au, ad)

        for i in range(tb // sub):
            r = pl.ds(i * sub, sub)
            av, dv = a_ref[r, :], dy_ref[r, :]
            hid[r, :], dg_ref[r, :], du_ref[r, :] = split(dot(av, gu_ref[0]), dot(av, gu_ref[1]), dot_nt(dv, wd_ref[...]))
        scheduled(phase, nf, t, nt, plan, stage_of, 1, 2)
        accumulate(ad, dy_ref[...].T, hid, 7)
        at = a_ref[...].T
        accumulate(ag, at, dg_ref, 7)
        accumulate(au, at, du_ref, 7)

        def give(ref):
            for i, acc in enumerate((ag, au)):
                ref[i] = acc[...].astype(BF16)

        @pl.when(t == nt - 1)
        def _():
            transposed(od_ref, ad)

        @pl.when((t == nt - 1) & (phase < done))
        def _():
            give(terms.at[phase])

        @pl.when((t == nt - 1) & (phase == done))
        def _():
            give(last_ref)
            for k, stage in leftover(plan, 2 * last + 1):
                stage_of(k, stage)
            for k in range(done):
                piece(k).sent()

    rows = row_blocks(tb, d)
    down = block((fc, d), lambda p, t: (p, 0))
    chunks = block((tb, fc), lambda p, t: (t, p))
    summed = (2, rows_d, done * fc)
    return pl.pallas_call(
        kernel,
        grid=(nf, nt),
        in_specs=[rows, rows, block((2, d, fc), lambda p, t: (0, 0, p)), down],
        out_specs=[chunks, chunks, fixed(2, d, fc), down, fixed(*summed), fixed(8, LANES)],
        out_shape=[shape(t_, f), shape(t_, f), shape(2, d, fc), shape(f, d), shape(*summed), shape(8, LANES, dtype=F32)],
        scratch_shapes=[pltpu.VMEM((tb, fc), BF16)]
        + [pltpu.VMEM((d, fc), F32)] * 3
        + [pltpu.VMEM((done, 2, d, fc), BF16)]
        + Sum.scratch(sizes["r"], rows_d, fc) * done,
        compiler_params=params(collective_id=1, has_side_effects=True),
        name="backward_top",
    )(a, dy, gu, wd)


def middle(sizes, dg, du, gu, h, dy, hid, d1, last, tb=512, sub=256):
    t_, f = dg.shape
    d = h.shape[1]
    nt = t_ // tb
    n_s = sizes["s"]
    rows_d, rows_f = d // n_s, f // n_s // 2
    d1 = d1.reshape(2 * n_s, rows_f, d)
    pieces = [(rows_f, WIDE), (rows_f, d - WIDE), (rows_d, last.shape[2])]
    plan = {k: (2, 4, 9, 11, 14, 2 * nt) if k > 1 else (2, 3, 7, 9, 12, 15) for k in range(len(pieces))}

    def kernel(dg_ref, du_ref, gu_ref, h_ref, dy_ref, hid_ref, d1_ref, last_ref, dh_ref, od_ref, s_ref, sd_ref, sq_ref, *scratch):
        ad, local = scratch[:2]
        phase, t = place_in_grid()
        place = Place(sizes)
        wide, right = pl.ds(0, WIDE), pl.ds(WIDE, d - WIDE)

        def stored(k):
            own = scratch[2 + k]
            sems = local.at[k]
            return (
                lambda: Stored(place, d1_ref, own, sems, wide),
                lambda: Stored(place, d1_ref, own, sems, right),
                lambda: Stored(place, last_ref, own, sems),
            )[k]()

        def piece(k):
            out = (sd_ref.at[:, :, wide], sd_ref.at[:, :, right], s_ref)[k]
            return Sum(place, *stored(k).terms(), out, sq_ref, parts_of(scratch[2 + len(pieces) :], len(pieces))[k])

        @pl.when(t == 0)
        def _():
            zero(ad, sq_ref)
            for k in plan:
                for one in stored(k).copies():
                    one.start()
            greet(place.around)

        @pl.when(t == 1)
        def _():
            for k in plan:
                for one in stored(k).copies():
                    one.wait()
            met(place.around)

        def stage_of(k, stage):
            piece(k).stages()[stage]()

        scheduled(phase, 1, t, nt, plan, stage_of, 0, 2)
        for i in range(tb // sub):
            r = pl.ds(i * sub, sub)
            da = dot_nt(gu_ref[0], dg_ref[r, :]).astype(BF16) + dot_nt(gu_ref[1], du_ref[r, :]).astype(BF16)
            da = da.T.astype(F32)
            wide_h = h_ref[r, :].astype(F32)
            scale = rms(wide_h)
            back = scale * da - wide_h * (scale * scale * scale * jnp.mean(da * wide_h, -1, keepdims=True))
            dh_ref[r, :] = dy_ref[r, :] + back.astype(BF16)
        scheduled(phase, 1, t, nt, plan, stage_of, 1, 2)
        accumulate(ad, dh_ref[...].T, hid_ref, 2)

        @pl.when(t == nt - 1)
        def _():
            transposed(od_ref, ad)
            for k, stage in leftover(plan, 2 * nt - 1):
                stage_of(k, stage)
            for k in plan:
                piece(k).sent()

    rows = lambda n: row_blocks(tb, n)
    summed = (2,) + pieces[2]
    scratch = [pltpu.VMEM((d, f), F32), DMA((len(pieces), 4))] + [pltpu.VMEM((4, 2) + p, BF16) for p in pieces]
    for p in pieces:
        scratch += Sum.scratch(sizes["r"], *p)
    return pl.pallas_call(
        kernel,
        grid=(1, nt),
        in_specs=[rows(f), rows(f), fixed(2, d, f), rows(d), rows(d), rows(f), ANY, ANY],
        out_specs=[rows(d), fixed(f, d), fixed(*summed), fixed(2, rows_f, d), fixed(8, LANES)],
        out_shape=[shape(t_, d), shape(f, d), shape(*summed), shape(2, rows_f, d), shape(8, LANES, dtype=F32)],
        scratch_shapes=scratch,
        compiler_params=params(collective_id=2, has_side_effects=True),
        name="middle",
    )(dg, du, gu, h, dy, hid, d1, last)


def backward_bottom(sizes, a, dy, by_gate, by_up, by_gate_n, by_up_n, wd, d0, sq1, sq2, tb=1024, sub=256):
    t_, d = a.shape
    f = wd.shape[0]
    nf, nt = f // WIDE, t_ // tb
    n_s = sizes["s"]
    rows_d, rows_f = d // n_s, f // n_s // 2
    d0 = d0.reshape(2 * n_s, rows_f, d)
    pieces = [(rows_d, WIDE)] * nf + [(rows_d, NARROW), (rows_f, WIDE), (rows_f, d - WIDE)]
    last = (nf + 1) * nt - 1
    slow = (0, 1, 4, 6, 9, 11)
    plan = {nf: after(last + 1, (0, 1, 4, 6, 8, 9)), nf + 1: after(1, slow), nf + 2: after(2, slow), 0: after(nt, slow)}
    plan |= {k: after((k + 1) * nt, (0, 1, 3, 5, 8, 10)) for k in range(1, nf)}

    def kernel(a_ref, dy_ref, gate_ref, up_ref, by_gaten_ref, by_upn_ref, wd_ref, d0_ref, sq1_ref, sq2_ref, s_ref, sd_ref, sum_ref, *scratch):
        dgu, acc, own0, own1, terms, terms_n, sq, squares, local, send, recv = scratch[:11]
        phase, t = place_in_grid()
        step = phase * nt + t
        place = Place(sizes)
        wide, right = pl.ds(0, WIDE), pl.ds(WIDE, d - WIDE)
        stored = lambda k: Stored(place, d0_ref, (own0, own1)[k], local.at[k], (wide, right)[k])

        def piece(k):
            part = parts_of(scratch[11:], len(pieces))[k]
            if k > nf:
                return Sum(place, *stored(k - nf - 1).terms(), sd_ref.at[:, :, (wide, right)[k - nf - 1]], sq, part)
            out = s_ref.at[:, :, pl.ds(k * WIDE, pieces[k][1])]
            return Sum(place, *term_blocks(terms.at[k] if k < nf else terms_n, place, rows_d), out, sq, part)

        others = [{"s": lax.rem(place.me + i, n_s)} for i in range(1, n_s)]

        def square_copies():
            return [
                pltpu.make_async_remote_copy(
                    src_ref=sq, dst_ref=squares.at[place.me], send_sem=send.at[i], recv_sem=recv.at[i], device_id=to, device_id_type=MESH
                )
                for i, to in enumerate(others)
            ]

        @pl.when(step == 0)
        def _():
            sq[...] = sq1_ref[...] + sq2_ref[...]
            for k in range(2):
                for one in stored(k).copies():
                    one.start()
            greet(others + [place.up, place.down])

        @pl.when(step == 1)
        def _():
            for k in range(2):
                for one in stored(k).copies():
                    one.wait()
            met(others + [place.up, place.down])

        scheduled(phase, nf + 1, t, nt, plan, lambda k, stage: piece(k).stages()[stage]())

        @pl.when(t == 0)
        def _():
            zero(acc)

        def work(width, gate_ref, up_ref):
            both = pl.ds(0, 2 * width)
            for i in range(tb // sub):
                r = pl.ds(i * sub, sub)
                dh = dot_nt(dy_ref[r, :], wd_ref[pl.ds(0, width), :])
                dh = dh.astype(BF16).astype(F32)
                for one, ref in enumerate((gate_ref, up_ref)):
                    dgu[r, pl.ds(one * width, width)] = (dh * ref[r, :]).astype(BF16)
            acc[:, both] += dot(a_ref[...].T, dgu[:, both])

        @pl.when(phase < nf)
        def _():
            work(WIDE, gate_ref, up_ref)

        @pl.when(phase == nf)
        def _():
            work(NARROW, by_gaten_ref, by_upn_ref)

        @pl.when((t == nt - 1) & (phase < nf))
        def _():
            for i in range(2):
                terms[phase, i] = acc[:, i * WIDE : (i + 1) * WIDE].astype(BF16)

        @pl.when(step == last)
        def _():
            for i in range(2):
                terms_n[i] = acc[:, i * NARROW : (i + 1) * NARROW].astype(BF16)
            for k, stage in leftover(plan, last):
                piece(k).stages()[stage]()
            for one in square_copies():
                one.start()
            squares[place.me] = sq[...]
            for one in square_copies():
                one.wait_recv()
            sum_ref[...] = sum(squares[i] for i in range(n_s))
            for k in range(len(pieces)):
                piece(k).sent()
            for one in square_copies():
                one.wait_send()

    rows = row_blocks(tb, d)
    chunks = block((None, tb, WIDE), lambda p, t: (jnp.minimum(p, nf - 1), jnp.where(p < nf, t, nt - 1), 0))
    narrow = block((tb, NARROW), lambda p, t: (jnp.where(p < nf, 0, t), 0))
    lanes = (8, LANES)
    scratch = [pltpu.VMEM((tb, 2 * WIDE), BF16), pltpu.VMEM((d, 2 * WIDE), F32)]
    scratch += [pltpu.VMEM((4, 2) + p, BF16) for p in pieces[nf + 1 :]]
    scratch += [pltpu.VMEM((nf, 2, d, WIDE), BF16), pltpu.VMEM((2, d, NARROW), BF16), pltpu.VMEM(lanes, F32), pltpu.VMEM((n_s,) + lanes, F32)]
    scratch += [DMA((2, 4)), DMA((n_s - 1,)), DMA((n_s - 1,))]
    for p in pieces:
        scratch += Sum.scratch(sizes["r"], *p)
    return pl.pallas_call(
        kernel,
        grid=(nf + 1, nt),
        in_specs=[rows, rows, chunks, chunks, narrow, narrow, block((WIDE, d), lambda p, t: (p, 0)), ANY, fixed(*lanes), fixed(*lanes)],
        out_specs=[fixed(2, rows_d, f), fixed(2, rows_f, d), fixed(*lanes)],
        out_shape=[shape(2, rows_d, f), shape(2, rows_f, d), shape(*lanes, dtype=F32)],
        scratch_shapes=scratch,
        compiler_params=params(collective_id=3, has_side_effects=True),
        name="backward_bottom",
    )(a, dy, by_gate, by_up, by_gate_n, by_up_n, wd, d0, sq1, sq2)


def update(sizes, weights, m, v, s0, s1, s1_end, sd0, sd1, squares):
    layers = weights[0].shape[0]
    sd0, sd1 = (one.reshape(weights[2].shape[1:]) for one in (sd0, sd1))
    count = sizes["s"] * sum(w.size for w in weights)
    early = s1.shape[2]
    arrays = (*weights, *m, *v)
    n = len(arrays)
    kinds = len(weights)

    sums = (s0, s1, s1_end, sd0, sd1)

    def kernel(sq_ref, *refs):
        far, refs = refs[: len(sums)], refs[len(sums) :]
        ins, outs, held, near, (arrive, leave, come) = refs[:n], refs[n : 2 * n], refs[2 * n : 3 * n], refs[3 * n : -3], refs[-3:]
        s0_ref, s1_ref, s1e_ref, sd0_ref, sd1_ref = near
        order = [(i, layer) for layer in range(layers) for i in range(kinds)]
        first = [pltpu.make_async_copy(src, dst, come.at[i]) for i, (src, dst) in enumerate(zip(far, near, strict=True))]
        for one in first:
            one.start()

        def copies(i, layer, back=False):
            out = []
            for k in range(i, n, kinds):
                src, dst, sem = (held[k], outs[k], leave) if back else (ins[k], held[k], arrive)
                out.append(pltpu.make_async_copy(src.at[layer], dst.at[layer], sem.at[k, layer]))
            return out

        for i, layer in order:
            for one in copies(i, layer):
                one.start()
        factor = jnp.minimum(1.0, 0.5 * lax.rsqrt(jnp.sum(sq_ref[...], keepdims=True) / count + 1e-30))
        for one in first:
            one.wait()
        for i, layer in order:
            for one in copies(i, layer):
                one.wait()
            w_ref, m_ref, v_ref = held[i::kinds]

            def change(g, cols, r):
                g = g[r, :].astype(F32) * factor
                new_m = 0.9 * m_ref[layer, r, cols] + 0.1 * g
                new_v = 0.95 * v_ref[layer, r, cols] + 0.05 * g * g
                w = w_ref[layer, r, cols].astype(F32)
                w_ref[layer, r, cols] = (w - 0.02 * (new_m * lax.rsqrt(new_v + 1e-8) + 0.1 * w)).astype(BF16)
                m_ref[layer, r, cols] = new_m
                v_ref[layer, r, cols] = new_v

            rows, width = w_ref.shape[1:]
            if i == kinds - 1:
                parts = [((sd0_ref, sd1_ref)[layer], pl.ds(0, width))]
            elif layer == 0:
                parts = [(s0_ref.at[i], pl.ds(0, width))]
            else:
                parts = [(s1_ref.at[i], pl.ds(0, early)), (s1e_ref.at[i], pl.ds(early, width - early))]
            for g, cols in parts:
                each(rows, lambda r, g=g, cols=cols: change(g, cols, r))
            for one in copies(i, layer, True):
                one.start()
        for i, layer in order:
            for one in copies(i, layer, True):
                one.wait()

    return pl.pallas_call(
        kernel,
        in_specs=[pl.BlockSpec(memory_space=pltpu.VMEM)] + [ANY] * (len(sums) + n),
        out_specs=[ANY] * n,
        out_shape=[jax.ShapeDtypeStruct(one.shape, one.dtype) for one in arrays],
        scratch_shapes=[pltpu.VMEM(one.shape, one.dtype) for one in arrays + sums] + [DMA((n, layers))] * 2 + [DMA((len(sums),))],
        compiler_params=pltpu.CompilerParams(vmem_limit_bytes=VMEM_LIMIT),
        name="update",
    )(squares, *sums, *arrays)


def solution(mesh):
    sizes = dict(mesh.shape)

    def step(x, dy, *arrays):
        weights, m, v = (arrays[i : i + 3] for i in (0, 3, 6))
        x, dy = x[0], dy[0]
        *slopes, h1, a1, a0, hid, wd0, wd1, gu1 = forward(sizes, x, *weights)
        dg, du, last, d1, s1, sq1 = backward_top(sizes, a1, dy, gu1, wd1)
        dh1, d0, s1_end, sd1, sq2 = middle(sizes, dg, du, gu1, h1, dy, hid, d1, last)
        s0, sd0, squares = backward_bottom(sizes, a0, dh1, *slopes, wd0, d0, sq1, sq2)
        return tuple(update(sizes, weights, m, v, s0, s1, s1_end, sd0, sd1, squares))

    states, cut = P(("rep", "r", "s"), None, None), P(None, "s", None)
    return jax.shard_map(
        step,
        mesh=mesh,
        in_specs=(states, states) + (cut,) * 9,
        out_specs=(P("rep", "s", None),) * 9,
        check_vma=False,
    )
```
